8 devices in a mesh: dp: 1 (over z), tpx: 2 (over y), tpy: 4 (over x, core).
Axes of the slice: x: 2, y: 2, z: 1, core: 2. Of those that a mesh axis runs over, the one named last changes fastest.
Arguments:
- hidden: bfloat16 [256, 4096], P('dp', ('tpx', 'tpy'))
- ln_scale: float32 [4096], P(('tpx', 'tpy'))
- w_q: bfloat16 [4096, 4096], P('tpx', 'tpy')
- w_k: bfloat16 [4096, 256], P('tpx')
- w_v: bfloat16 [4096, 256], P('tpx')
- w_gate: bfloat16 [4096, 16384], P('tpx', 'tpy')
- w_up: bfloat16 [4096, 16384], P('tpx', 'tpy')
- w_o: bfloat16 [4096, 4096], P('tpy', 'tpx')
- w_down: bfloat16 [16384, 4096], P('tpy', 'tpx')
- k_cache: bfloat16 [256, 2048, 256], P(('dp', 'tpx', 'tpy'))
- v_cache: bfloat16 [256, 2048, 256], P(('dp', 'tpx', 'tpy'))
- positions: int32 [256], P(('dp', 'tpx', 'tpy'))
Outputs:
- output 1: bfloat16 [256, 4096], P('dp', ('tpx', 'tpy'))
- output 2: bfloat16 [256, 2048, 256], P(('dp', 'tpx', 'tpy'))
- output 3: bfloat16 [256, 2048, 256], P(('dp', 'tpx', 'tpy'))
All inputs are finite; a program needn't handle non-finite values.
Results may differ from the reference program's by a relative error of at most 0.00648642.
Values are sent between devices in bfloat16 or wider.
A program may use at most 1 GiB of HBM per device.

```python
import math
import jax
import jax.numpy as jnp
from jax import lax

D_MODEL = 4096
N_HEADS = 16
HEAD_DIM = 256
FF_DIM = 16384
SEQ_COUNT = 256
CACHE_LEN = 2048


def draw_positions(len_key, perm_key):
    pos_draw = jax.random.randint(len_key, (SEQ_COUNT,), 200, CACHE_LEN)
    seq_order = jax.random.permutation(perm_key, SEQ_COUNT)
    seq_ids = jnp.arange(SEQ_COUNT)
    positions = jnp.where(seq_ids == seq_order[0], CACHE_LEN - 1, pos_draw)
    positions = jnp.where(seq_ids == seq_order[1], 200, positions)
    return positions.astype(jnp.int32)


def setup_inputs(seed: int = 0, part: int = 0) -> dict:
    root_key = jax.random.key(seed)
    part_keys = jax.random.split(jax.random.fold_in(root_key, part), 8)
    shared_keys = jax.random.split(root_key, 8)
    d_scale = D_MODEL ** -0.5
    col_scale = 0.5 + 1.5 * jnp.arange(D_MODEL, dtype=jnp.float32) / D_MODEL
    hidden = 0.5 + col_scale * jax.random.normal(part_keys[0], (SEQ_COUNT, D_MODEL), jnp.float32)
    ln_scale = jax.random.uniform(shared_keys[0], (D_MODEL,), jnp.float32, 0.5, 1.5)
    w_k = jax.random.normal(shared_keys[1], (D_MODEL, HEAD_DIM), jnp.float32) * d_scale
    align_coef = min(0.9, math.log(CACHE_LEN / 2) / math.sqrt(HEAD_DIM))
    noise_coef = math.sqrt(1.0 - align_coef * align_coef)
    q_noise = jax.random.normal(shared_keys[2], (D_MODEL, N_HEADS, HEAD_DIM), jnp.float32) * d_scale
    w_q = (align_coef * w_k[:, None, :] + noise_coef * q_noise).reshape(D_MODEL, N_HEADS * HEAD_DIM)
    w_v = jax.random.normal(shared_keys[3], (D_MODEL, HEAD_DIM), jnp.float32) * d_scale
    w_gate = jax.random.normal(shared_keys[4], (D_MODEL, FF_DIM), jnp.float32) * d_scale
    w_up = jax.random.normal(shared_keys[5], (D_MODEL, FF_DIM), jnp.float32) * d_scale
    w_o = jax.random.normal(shared_keys[6], (N_HEADS * HEAD_DIM, D_MODEL), jnp.float32) * (N_HEADS * HEAD_DIM) ** -0.5
    w_down = jax.random.normal(shared_keys[7], (FF_DIM, D_MODEL), jnp.float32) * FF_DIM ** -0.5
    k_cache = jax.random.normal(part_keys[1], (SEQ_COUNT, CACHE_LEN, HEAD_DIM), jnp.float32)
    seq_mean = jax.random.normal(part_keys[2], (SEQ_COUNT, 1, HEAD_DIM), jnp.float32)
    v_cache = seq_mean + 0.5 * jax.random.normal(part_keys[3], (SEQ_COUNT, CACHE_LEN, HEAD_DIM), jnp.float32)
    positions = draw_positions(part_keys[4], part_keys[5])
    return {
        'hidden': hidden.astype(jnp.bfloat16),
        'ln_scale': ln_scale,
        'w_q': w_q.astype(jnp.bfloat16),
        'w_k': w_k.astype(jnp.bfloat16),
        'w_v': w_v.astype(jnp.bfloat16),
        'w_gate': w_gate.astype(jnp.bfloat16),
        'w_up': w_up.astype(jnp.bfloat16),
        'w_o': w_o.astype(jnp.bfloat16),
        'w_down': w_down.astype(jnp.bfloat16),
        'k_cache': k_cache.astype(jnp.bfloat16),
        'v_cache': v_cache.astype(jnp.bfloat16),
        'positions': positions,
    }


def rope_tables(positions):
    half_dim = HEAD_DIM // 2
    inv_freq = 10000.0 ** (-(jnp.arange(half_dim, dtype=jnp.float32) * 2.0 / HEAD_DIM))
    angles = positions.astype(jnp.float32)[:, None] * inv_freq[None, :]
    return jnp.cos(angles), jnp.sin(angles)


def apply_rope(vectors, cos_tab, sin_tab):
    half_dim = HEAD_DIM // 2
    lead_half = vectors[..., :half_dim]
    tail_half = vectors[..., half_dim:]
    return jnp.concatenate([lead_half * cos_tab - tail_half * sin_tab, lead_half * sin_tab + tail_half * cos_tab], axis=-1)


def reference(hidden, ln_scale, w_q, w_k, w_v, w_gate, w_up, w_o, w_down, k_cache, v_cache, positions):
    hidden_f = hidden.astype(jnp.float32)
    mean_val = jnp.mean(hidden_f, axis=1, keepdims=True)
    var_val = jnp.mean(jnp.square(hidden_f - mean_val), axis=1, keepdims=True)
    normed = ((hidden_f - mean_val) * lax.rsqrt(var_val + 1e-6) * ln_scale).astype(jnp.bfloat16)
    q_proj = jnp.dot(normed, w_q, preferred_element_type=jnp.float32).astype(jnp.bfloat16)
    k_proj = jnp.dot(normed, w_k, preferred_element_type=jnp.float32).astype(jnp.bfloat16)
    v_proj = jnp.dot(normed, w_v, preferred_element_type=jnp.float32).astype(jnp.bfloat16)
    gate_proj = jnp.dot(normed, w_gate, preferred_element_type=jnp.float32).astype(jnp.bfloat16)
    up_proj = jnp.dot(normed, w_up, preferred_element_type=jnp.float32).astype(jnp.bfloat16)
    mlp_act = (jax.nn.silu(gate_proj.astype(jnp.float32)) * up_proj.astype(jnp.float32)).astype(jnp.bfloat16)
    mlp_out = jnp.dot(mlp_act, w_down, preferred_element_type=jnp.float32)
    cos_tab, sin_tab = rope_tables(positions)
    q_heads = q_proj.astype(jnp.float32).reshape(SEQ_COUNT, N_HEADS, HEAD_DIM)
    q_rot = apply_rope(q_heads, cos_tab[:, None, :], sin_tab[:, None, :]).astype(jnp.bfloat16)
    k_rot = apply_rope(k_proj.astype(jnp.float32), cos_tab, sin_tab).astype(jnp.bfloat16)
    is_new = jnp.arange(CACHE_LEN)[None, :, None] == positions[:, None, None]
    k_out = jnp.where(is_new, k_rot[:, None, :], k_cache)
    v_out = jnp.where(is_new, v_proj[:, None, :], v_cache)

    def one_sequence(seq_item):
        q_seq, k_seq, v_seq, pos_seq = seq_item
        scores = jnp.dot(q_seq, k_seq.T, preferred_element_type=jnp.float32) * (HEAD_DIM ** -0.5)
        valid_rows = jnp.arange(CACHE_LEN)[None, :] <= pos_seq
        scores = jnp.where(valid_rows, scores, -jnp.inf)
        attn_prob = jax.nn.softmax(scores, axis=-1).astype(jnp.bfloat16)
        return jnp.dot(attn_prob, v_seq, preferred_element_type=jnp.float32).astype(jnp.bfloat16)

    attn_heads = lax.map(one_sequence, (q_rot, k_out, v_out, positions))
    attn_out = jnp.dot(attn_heads.reshape(SEQ_COUNT, N_HEADS * HEAD_DIM), w_o, preferred_element_type=jnp.float32)
    hidden_out = (hidden_f + attn_out + mlp_out).astype(jnp.bfloat16)
    return (hidden_out, k_out, v_out)
```

```python
import functools

import jax
import jax.numpy as jnp
from jax import lax
from jax.experimental import pallas as pl
from jax.experimental.pallas import tpu as pltpu
from jax.sharding import PartitionSpec as P

LN_EPS = 1e-6
ROPE_BASE = 10000.0
MESH = pl.DeviceIdType.MESH
F32 = jnp.float32
BF16 = jnp.bfloat16


def rope_tables(positions, head_dim):
    half_dim = head_dim // 2
    inv_freq = ROPE_BASE ** (-(jnp.arange(half_dim, dtype=F32) * 2.0 / head_dim))
    angles = positions.astype(F32)[:, None] * inv_freq[None, :]
    return jnp.cos(angles), jnp.sin(angles)


def rope(x, cos, sin):
    half = x.shape[-1] // 2
    lead, tail = x[:, :half], x[:, half:]
    return jnp.concatenate([lead * cos - tail * sin, lead * sin + tail * cos], axis=-1)


def front_kernel(nx, ny, h_ref, sc_ref, u_ref, hbuf, scbuf, stat, hs, hr, ss, sr, ts, tr):
    ix, iy = lax.axis_index("tpx"), lax.axis_index("tpy")
    rows, width = h_ref.shape
    partner = iy + 1 - 2 * lax.rem(iy, 2)
    cross = lax.rem(iy + 2, ny)
    diag = lax.rem(partner + 2, ny)
    me = ix * ny + iy

    barrier = pltpu.get_barrier_semaphore()
    for dx in range(nx):
        for dy in range(ny):
            if dx or dy:
                pl.semaphore_signal(
                    barrier,
                    inc=1,
                    device_id={"tpx": lax.rem(ix + dx, nx), "tpy": lax.rem(iy + dy, ny)},
                    device_id_type=MESH,
                )
    pl.semaphore_wait(barrier, nx * ny - 1)

    half = rows // 2

    def block_copy(src, owner, part, dst_y, k):
        sl = pl.ds(part * half, half)
        return pltpu.make_async_remote_copy(
            src_ref=src.at[sl],
            dst_ref=hbuf.at[owner, sl],
            send_sem=hs.at[k, part],
            recv_sem=hr.at[k, part],
            device_id={"tpx": ix, "tpy": dst_y},
            device_id_type=MESH,
        )

    to_cross = [block_copy(h_ref, iy, p, cross, 0) for p in range(2)]
    to_partner = [block_copy(h_ref, iy, p, partner, 1) for p in range(2)]
    for c in to_cross + to_partner:
        c.start()
    sc_copies = []
    for k, dst in enumerate((cross, partner, diag)):
        c = pltpu.make_async_remote_copy(
            src_ref=sc_ref,
            dst_ref=scbuf.at[iy],
            send_sem=ss.at[k],
            recv_sem=sr.at[k],
            device_id={"tpx": ix, "tpy": dst},
            device_id_type=MESH,
        )
        c.start()
        sc_copies.append(c)

    hf = h_ref[...].astype(F32)
    total = jnp.sum(hf, axis=1, keepdims=True)
    dev = hf - total / width
    spread = jnp.sum(dev * dev, axis=1, keepdims=True)
    lane = lax.broadcasted_iota(jnp.int32, (rows, 128), 1)
    packed = jnp.where(lane == 0, total, jnp.where(lane == 1, spread, 0.0))
    stat[me] = jnp.transpose(packed)[:8]

    stat_copies = []
    k = 0
    for dx in range(nx):
        for dy in range(ny):
            if dx or dy:
                c = pltpu.make_async_remote_copy(
                    src_ref=stat.at[me],
                    dst_ref=stat.at[me],
                    send_sem=ts.at[k],
                    recv_sem=tr.at[k],
                    device_id={"tpx": lax.rem(ix + dx, nx), "tpy": lax.rem(iy + dy, ny)},
                    device_id_type=MESH,
                )
                c.start()
                stat_copies.append(c)
                k += 1

    forward = []
    for p in range(2):
        to_cross[p].wait_recv()
        c = pltpu.make_async_remote_copy(
            src_ref=hbuf.at[cross, pl.ds(p * half, half)],
            dst_ref=hbuf.at[cross, pl.ds(p * half, half)],
            send_sem=hs.at[2, p],
            recv_sem=hr.at[2, p],
            device_id={"tpx": ix, "tpy": partner},
            device_id_type=MESH,
        )
        c.start()
        forward.append(c)

    for c in stat_copies:
        c.wait_recv()
    n_dev = nx * ny
    sums = [stat[d, 0:1, :] for d in range(n_dev)]
    sprd = [stat[d, 1:2, :] for d in range(n_dev)]
    mean = functools.reduce(jnp.add, sums) / (width * n_dev)
    m2 = functools.reduce(jnp.add, sprd)
    for d in range(n_dev):
        gap = sums[d] / width - mean
        m2 = m2 + width * gap * gap
    var = m2 / (width * n_dev)
    rs = lax.rsqrt(var + LN_EPS)
    sub = lax.broadcasted_iota(jnp.int32, (128, rows), 0)
    cols = jnp.transpose(jnp.where(sub == 0, mean, jnp.where(sub == 1, rs, 0.0)))
    mean_c, rs_c = cols[:, 0:1], cols[:, 1:2]

    def emit(block, scale, owner):
        u = ((block.astype(F32) - mean_c) * rs_c * scale).astype(BF16)
        col = pl.ds(pl.multiple_of(owner * width, width), width)
        for hf_i in range(2):
            pos = lax.rem(hf_i + ix + 1, 2)
            u_ref[pl.ds(pl.multiple_of(pos * half, half), half), col] = u[hf_i * half : (hf_i + 1) * half]

    emit(h_ref[...], sc_ref[...], iy)
    for c in sc_copies:
        c.wait_recv()
    for c in to_partner:
        c.wait_recv()
    emit(hbuf[partner], scbuf[partner], partner)
    emit(hbuf[cross], scbuf[cross], cross)
    for c in forward:
        c.wait_recv()
    emit(hbuf[diag], scbuf[diag], diag)
    for c in to_cross + to_partner + forward + sc_copies + stat_copies:
        c.wait_send()


def front(nx, ny, hidden, ln_scale):
    rows, width = hidden.shape
    n_dev = nx * ny
    return pl.pallas_call(
        functools.partial(front_kernel, nx, ny),
        out_shape=jax.ShapeDtypeStruct((rows, width * ny), BF16),
        in_specs=[pl.BlockSpec(memory_space=pltpu.VMEM)] * 2,
        out_specs=pl.BlockSpec(memory_space=pltpu.VMEM),
        scratch_shapes=[
            pltpu.VMEM((ny, rows, width), BF16),
            pltpu.VMEM((ny, 1, width), F32),
            pltpu.VMEM((n_dev, 8, rows), F32),
            pltpu.SemaphoreType.DMA((3, 2)),
            pltpu.SemaphoreType.DMA((3, 2)),
            pltpu.SemaphoreType.DMA((3,)),
            pltpu.SemaphoreType.DMA((3,)),
            pltpu.SemaphoreType.DMA((n_dev - 1,)),
            pltpu.SemaphoreType.DMA((n_dev - 1,)),
        ],
        compiler_params=pltpu.CompilerParams(collective_id=0, has_side_effects=True),
        cost_estimate=pl.CostEstimate(flops=10**9, bytes_accessed=2 * 10**6, transcendentals=0),
        name="front",
    )(hidden, ln_scale.reshape(1, width))


def gu_kernel(n_chunk, per, u_ref, wg_ref, wu_ref, *outs):
    i = pl.program_id(0)
    half = u_ref.shape[0] // 2
    g = jnp.dot(u_ref[...], wg_ref[...], preferred_element_type=F32)
    w = jnp.dot(u_ref[...], wu_ref[...], preferred_element_type=F32)
    for c in range(n_chunk):
        send, keep = outs[c], outs[n_chunk + c]

        @pl.when(i // per == c)
        def _():
            send[0] = g[:half]
            send[1] = w[:half]
            keep[0] = g[half:]
            keep[1] = w[half:]


def gate_up(u, w_gate, w_up, n_chunk, blk):
    rows, kdim = u.shape
    cols = w_gate.shape[1]
    steps = cols // blk
    per = steps // n_chunk
    half = rows // 2

    def omap(c):
        return lambda i: (0, 0, jnp.clip(i - c * per, 0, per - 1))

    out = pl.BlockSpec
    shape = jax.ShapeDtypeStruct((2, half, cols // n_chunk), F32)
    res = pl.pallas_call(
        functools.partial(gu_kernel, n_chunk, per),
        grid=(steps,),
        out_shape=[shape] * (2 * n_chunk),
        in_specs=[
            pl.BlockSpec((rows, kdim), lambda i: (0, 0)),
            pl.BlockSpec((kdim, blk), lambda i: (0, i)),
            pl.BlockSpec((kdim, blk), lambda i: (0, i)),
        ],
        out_specs=[out((2, half, blk), omap(c % n_chunk)) for c in range(2 * n_chunk)],
        compiler_params=pltpu.CompilerParams(vmem_limit_bytes=48 * 2**20),
        cost_estimate=pl.CostEstimate(
            flops=4 * rows * kdim * cols, bytes_accessed=4 * kdim * cols, transcendentals=0
        ),
        name="gate_up",
    )(u, w_gate, w_up)
    return res[:n_chunk], res[n_chunk:]


def attn_kernel(nb, ahead, pos_ref, q_ref, kn_ref, vn_ref, cos_ref, sin_ref, kc_ref, vc_ref,
                o_ref, ko_ref, vo_ref, kbuf, vbuf, krow, vrow, ki, vi, ks, vs):
    n_seq, n_head, dim = q_ref.shape
    length = kbuf.shape[1]

    def fetch(b, slot):
        pltpu.make_async_copy(kc_ref.at[b], kbuf.at[slot], ki.at[slot]).start()
        pltpu.make_async_copy(vc_ref.at[b], vbuf.at[slot], vi.at[slot]).start()

    def wait_out(b, slot):
        pltpu.make_async_copy(kbuf.at[slot], ko_ref.at[b], ks.at[slot]).wait()
        pltpu.make_async_copy(vbuf.at[slot], vo_ref.at[b], vs.at[slot]).wait()

    for b in range(ahead):
        fetch(b, b)
    krow[...] = rope(kn_ref[...].astype(F32), cos_ref[...], sin_ref[...]).astype(BF16).astype(F32)
    vrow[...] = vn_ref[...].astype(F32)

    def patch(buf, slot, row, p):
        base = pl.multiple_of((p // 16) * 16, 16)
        old = buf[slot, pl.ds(base, 16), :].astype(F32)
        hit = lax.broadcasted_iota(jnp.int32, old.shape, 0) == p - base
        buf[slot, pl.ds(base, 16), :] = jnp.where(hit, row, old).astype(BF16)

    @pl.loop(0, n_seq // 2)
    def _(i):
        work = []
        for j in range(2):
            b = 2 * i + j
            slot = lax.rem(b, nb)
            nxt = b + ahead
            nslot = lax.rem(nxt, nb)

            @pl.when(jnp.logical_and(nxt < n_seq, nxt >= nb))
            def _():
                wait_out(nxt - nb, nslot)

            @pl.when(nxt < n_seq)
            def _():
                fetch(nxt, nslot)

            work.append((b, slot))
        for b, slot in work:
            p = pos_ref[b]
            pltpu.make_async_copy(kc_ref.at[b], kbuf.at[slot], ki.at[slot]).wait()
            patch(kbuf, slot, krow[pl.ds(b, 1), :], p)
            pltpu.make_async_copy(vc_ref.at[b], vbuf.at[slot], vi.at[slot]).wait()
            patch(vbuf, slot, vrow[pl.ds(b, 1), :], p)
        for b, slot in work:
            p = pos_ref[b]
            q = rope(q_ref[b].astype(F32), cos_ref[pl.ds(b, 1), :], sin_ref[pl.ds(b, 1), :]).astype(BF16)
            s = lax.dot_general(q, kbuf[slot], (((1,), (1,)), ((), ())), preferred_element_type=F32)
            s = s * (dim ** -0.5)
            ok = lax.broadcasted_iota(jnp.int32, (n_head, length), 1) <= p
            s = jnp.where(ok, s, -jnp.inf)
            e = jnp.exp(s - jnp.max(s, axis=1, keepdims=True))
            prob = (e / jnp.sum(e, axis=1, keepdims=True)).astype(BF16)
            o = jnp.dot(prob, vbuf[slot], preferred_element_type=F32)
            o_ref[b] = o.astype(BF16)
        for b, slot in work:
            pltpu.make_async_copy(kbuf.at[slot], ko_ref.at[b], ks.at[slot]).start()
            pltpu.make_async_copy(vbuf.at[slot], vo_ref.at[b], vs.at[slot]).start()

    for b in range(n_seq - nb, n_seq):
        wait_out(b, b % nb)


def attention(q, k_new, v_new, cos, sin, k_cache, v_cache, positions, nb=8, ahead=4):
    n_seq, length, dim = k_cache.shape
    n_head = q.shape[1]
    vm = pl.BlockSpec(memory_space=pltpu.VMEM)
    hbm = pl.BlockSpec(memory_space=pltpu.HBM)
    return pl.pallas_call(
        functools.partial(attn_kernel, nb, ahead),
        out_shape=[
            jax.ShapeDtypeStruct(q.shape, BF16),
            jax.ShapeDtypeStruct(k_cache.shape, BF16),
            jax.ShapeDtypeStruct(v_cache.shape, BF16),
        ],
        in_specs=[pl.BlockSpec(memory_space=pltpu.SMEM), vm, vm, vm, vm, vm, hbm, hbm],
        out_specs=[vm, hbm, hbm],
        scratch_shapes=[
            pltpu.VMEM((nb, length, dim), BF16),
            pltpu.VMEM((nb, length, dim), BF16),
            pltpu.VMEM((n_seq, dim), F32),
            pltpu.VMEM((n_seq, dim), F32),
            pltpu.SemaphoreType.DMA((nb,)),
            pltpu.SemaphoreType.DMA((nb,)),
            pltpu.SemaphoreType.DMA((nb,)),
            pltpu.SemaphoreType.DMA((nb,)),
        ],
        compiler_params=pltpu.CompilerParams(vmem_limit_bytes=32 * 2**20),
        cost_estimate=pl.CostEstimate(
            flops=4 * 10**10, bytes_accessed=8 * n_seq * length * dim, transcendentals=n_seq * n_head * length
        ),
        name="attention",
    )(positions, q, k_new, v_new, cos, sin, k_cache, v_cache)


def solution(mesh):
    x_size = mesh.shape["tpx"]
    y_size = mesh.shape["tpy"]
    hidden_spec = P("dp", ("tpx", "tpy"))
    cache_spec = P(("dp", "tpx", "tpy"), None, None)
    in_specs = (hidden_spec, P(("tpx", "tpy")), P("tpx", "tpy"), P("tpx", None), P("tpx", None), P("tpx", "tpy"), P("tpx", "tpy"), P("tpy", "tpx"), P("tpy", "tpx"), cache_spec, cache_spec, P(("dp", "tpx", "tpy")))
    out_specs = (hidden_spec, cache_spec, cache_spec)
    swap_x = [(0, 1), (1, 0)]
    swap_core = [(0, 1), (1, 0), (2, 3), (3, 2)]
    swap_chip = [(0, 2), (2, 0), (1, 3), (3, 1)]
    n_chunk = 4

    def device_step(hidden, ln_scale, w_q, w_k, w_v, w_gate, w_up, w_o, w_down, k_cache, v_cache, positions):
        ix, iy = lax.axis_index("tpx"), lax.axis_index("tpy")
        rows, width = hidden.shape
        half = rows // 2
        n_seq = positions.shape[0]
        dim = k_cache.shape[2]
        cols = w_gate.shape[1]

        def dot(a, b):
            return jnp.dot(a, b, preferred_element_type=F32)

        u = front(x_size, y_size, hidden, ln_scale)
        u_oth, u_own = u[:half], u[half:]
        q_send = dot(u_oth, w_q)
        kv_rows_oth = lax.dynamic_slice_in_dim(u_oth, iy * n_seq, n_seq, axis=0)
        kv_rows_own = lax.dynamic_slice_in_dim(u_own, iy * n_seq, n_seq, axis=0)
        kv_send = jnp.concatenate([dot(kv_rows_oth, w_k), dot(kv_rows_oth, w_v)], axis=1)
        q_recv = lax.ppermute(q_send, "tpx", swap_x)
        kv_recv = lax.ppermute(kv_send, "tpx", swap_x)
        q_own = dot(u_own, w_q)
        kv_own = jnp.concatenate([dot(kv_rows_own, w_k), dot(kv_rows_own, w_v)], axis=1)

        send, keep = gate_up(u, w_gate, w_up, n_chunk, 512)
        recv = [lax.ppermute(s, "tpx", swap_x) for s in send]

        q_heads = (q_own + q_recv).astype(BF16).reshape(half, -1, dim)
        kv_new = (kv_own + kv_recv).astype(BF16)
        q_seq = lax.all_to_all(q_heads, "tpy", 0, 1, tiled=True)
        cos_tab, sin_tab = rope_tables(positions, dim)
        attn_seq, k_all, v_all = attention(q_seq, kv_new[:, :dim], kv_new[:, dim:], cos_tab, sin_tab, k_cache, v_cache, positions)

        attn_heads = lax.all_to_all(attn_seq, "tpy", 1, 0, tiled=True)
        o_own = attn_heads.reshape(half, -1)
        o_oth = lax.ppermute(o_own, "tpx", swap_x)
        part = dot(jnp.concatenate([o_oth, o_own], axis=0), w_o)
        per = cols // n_chunk
        for c in range(n_chunk):
            gw = keep[c] + recv[c]
            gate = gw[0].astype(BF16).astype(F32)
            up = gw[1].astype(BF16).astype(F32)
            act_own = (jax.nn.silu(gate) * up).astype(BF16)
            act_oth = lax.ppermute(act_own, "tpx", swap_x)
            act = jnp.concatenate([act_oth, act_own], axis=0)
            part = part + dot(act, w_down[c * per : (c + 1) * per])

        blocks = part.reshape(rows, 2, 2, width)
        core, chip = lax.rem(iy, 2), iy // 2
        give = lax.dynamic_index_in_dim(blocks, 1 - core, 2, keepdims=False)
        hold = lax.dynamic_index_in_dim(blocks, core, 2, keepdims=False)
        pair = hold + lax.ppermute(give, "tpy", swap_core)
        give = lax.dynamic_index_in_dim(pair, 1 - chip, 1, keepdims=False)
        hold = lax.dynamic_index_in_dim(pair, chip, 1, keepdims=False)
        total = hold + lax.ppermute(give, "tpy", swap_chip)
        natural = jnp.where(ix == 0, jnp.concatenate([total[half:], total[:half]], axis=0), total)
        hidden_out = (hidden.astype(F32) + natural).astype(BF16)
        return hidden_out, k_all, v_all

    return jax.shard_map(device_step, mesh=mesh, in_specs=in_specs, out_specs=out_specs, check_vma=False)
```

```python
import functools

import jax
import jax.numpy as jnp
from jax import lax
from jax.experimental import pallas as pl
from jax.experimental.pallas import tpu as pltpu
from jax.sharding import PartitionSpec as P


LN_EPS = 1e-6
ROPE_BASE = 10000.0
MESH = pl.DeviceIdType.MESH
F32 = jnp.float32
BF16 = jnp.bfloat16


def rope_tables(positions, head_dim):
    half_dim = head_dim // 2
    inv_freq = ROPE_BASE ** (-(jnp.arange(half_dim, dtype=F32) * 2.0 / head_dim))
    angles = positions.astype(F32)[:, None] * inv_freq[None, :]
    return jnp.cos(angles), jnp.sin(angles)


def rope(x, cos, sin):
    half = x.shape[-1] // 2
    lead, tail = x[:, :half], x[:, half:]
    return jnp.concatenate([lead * cos - tail * sin, lead * sin + tail * cos], axis=-1)


def front_kernel(nx, ny, h_ref, sc_ref, u_ref, hbuf, scbuf, stat, hs, hr, ss, sr, ts, tr):
    ix, iy = lax.axis_index("tpx"), lax.axis_index("tpy")
    rows, width = h_ref.shape
    partner = iy + 1 - 2 * lax.rem(iy, 2)
    cross = lax.rem(iy + 2, ny)
    diag = lax.rem(partner + 2, ny)
    me = ix * ny + iy

    barrier = pltpu.get_barrier_semaphore()
    for dx in range(nx):
        for dy in range(ny):
            if dx or dy:
                pl.semaphore_signal(
                    barrier,
                    inc=1,
                    device_id={"tpx": lax.rem(ix + dx, nx), "tpy": lax.rem(iy + dy, ny)},
                    device_id_type=MESH,
                )
    pl.semaphore_wait(barrier, nx * ny - 1)

    half = rows // 2

    def block_copy(src, owner, part, dst_y, k):
        sl = pl.ds(part * half, half)
        return pltpu.make_async_remote_copy(
            src_ref=src.at[sl],
            dst_ref=hbuf.at[owner, sl],
            send_sem=hs.at[k, part],
            recv_sem=hr.at[k, part],
            device_id={"tpx": ix, "tpy": dst_y},
            device_id_type=MESH,
        )

    to_cross = [block_copy(h_ref, iy, p, cross, 0) for p in range(2)]
    to_partner = [block_copy(h_ref, iy, p, partner, 1) for p in range(2)]
    for c in to_cross + to_partner:
        c.start()
    sc_copies = []
    for k, dst in enumerate((cross, partner, diag)):
        c = pltpu.make_async_remote_copy(
            src_ref=sc_ref,
            dst_ref=scbuf.at[iy],
            send_sem=ss.at[k],
            recv_sem=sr.at[k],
            device_id={"tpx": ix, "tpy": dst},
            device_id_type=MESH,
        )
        c.start()
        sc_copies.append(c)

    hf = h_ref[...].astype(F32)
    total = jnp.sum(hf, axis=1, keepdims=True)
    dev = hf - total / width
    spread = jnp.sum(dev * dev, axis=1, keepdims=True)
    lane = lax.broadcasted_iota(jnp.int32, (rows, 128), 1)
    packed = jnp.where(lane == 0, total, jnp.where(lane == 1, spread, 0.0))
    stat[me] = jnp.transpose(packed)[:8]

    stat_copies = []
    k = 0
    for dx in range(nx):
        for dy in range(ny):
            if dx or dy:
                c = pltpu.make_async_remote_copy(
                    src_ref=stat.at[me],
                    dst_ref=stat.at[me],
                    send_sem=ts.at[k],
                    recv_sem=tr.at[k],
                    device_id={"tpx": lax.rem(ix + dx, nx), "tpy": lax.rem(iy + dy, ny)},
                    device_id_type=MESH,
                )
                c.start()
                stat_copies.append(c)
                k += 1

    forward = []
    for p in range(2):
        to_cross[p].wait_recv()
        c = pltpu.make_async_remote_copy(
            src_ref=hbuf.at[cross, pl.ds(p * half, half)],
            dst_ref=hbuf.at[cross, pl.ds(p * half, half)],
            send_sem=hs.at[2, p],
            recv_sem=hr.at[2, p],
            device_id={"tpx": ix, "tpy": partner},
            device_id_type=MESH,
        )
        c.start()
        forward.append(c)

    for c in stat_copies:
        c.wait_recv()
    n_dev = nx * ny
    sums = [stat[d, 0:1, :] for d in range(n_dev)]
    sprd = [stat[d, 1:2, :] for d in range(n_dev)]
    mean = functools.reduce(jnp.add, sums) / (width * n_dev)
    m2 = functools.reduce(jnp.add, sprd)
    for d in range(n_dev):
        gap = sums[d] / width - mean
        m2 = m2 + width * gap * gap
    var = m2 / (width * n_dev)
    rs = lax.rsqrt(var + LN_EPS)
    sub = lax.broadcasted_iota(jnp.int32, (128, rows), 0)
    cols = jnp.transpose(jnp.where(sub == 0, mean, jnp.where(sub == 1, rs, 0.0)))
    mean_c, rs_c = cols[:, 0:1], cols[:, 1:2]

    def emit(block, scale, owner):
        u = ((block.astype(F32) - mean_c) * rs_c * scale).astype(BF16)
        col = pl.ds(pl.multiple_of(owner * width, width), width)
        for hf_i in range(2):
            pos = lax.rem(hf_i + ix + 1, 2)
            u_ref[pl.ds(pl.multiple_of(pos * half, half), half), col] = u[hf_i * half : (hf_i + 1) * half]

    emit(h_ref[...], sc_ref[...], iy)
    for c in sc_copies:
        c.wait_recv()
    for c in to_partner:
        c.wait_recv()
    emit(hbuf[partner], scbuf[partner], partner)
    emit(hbuf[cross], scbuf[cross], cross)
    for c in forward:
        c.wait_recv()
    emit(hbuf[diag], scbuf[diag], diag)
    for c in to_cross + to_partner + forward + sc_copies + stat_copies:
        c.wait_send()


def front(nx, ny, hidden, ln_scale):
    rows, width = hidden.shape
    n_dev = nx * ny
    return pl.pallas_call(
        functools.partial(front_kernel, nx, ny),
        out_shape=jax.ShapeDtypeStruct((rows, width * ny), BF16),
        in_specs=[pl.BlockSpec(memory_space=pltpu.VMEM)] * 2,
        out_specs=pl.BlockSpec(memory_space=pltpu.VMEM),
        scratch_shapes=[
            pltpu.VMEM((ny, rows, width), BF16),
            pltpu.VMEM((ny, 1, width), F32),
            pltpu.VMEM((n_dev, 8, rows), F32),
            pltpu.SemaphoreType.DMA((3, 2)),
            pltpu.SemaphoreType.DMA((3, 2)),
            pltpu.SemaphoreType.DMA((3,)),
            pltpu.SemaphoreType.DMA((3,)),
            pltpu.SemaphoreType.DMA((n_dev - 1,)),
            pltpu.SemaphoreType.DMA((n_dev - 1,)),
        ],
        compiler_params=pltpu.CompilerParams(collective_id=0, has_side_effects=True),
        cost_estimate=pl.CostEstimate(flops=10**9, bytes_accessed=2 * 10**6, transcendentals=0),
        name="front",
    )(hidden, ln_scale.reshape(1, width))


def gu_kernel(u_ref, wg_ref, wu_ref, send, keep):
    half = u_ref.shape[0] // 2
    for k, w_ref in enumerate((wg_ref, wu_ref)):
        y = jnp.dot(u_ref[...], w_ref[...], preferred_element_type=F32)
        send[k] = y[:half]
        keep[k] = y[half:]


def gate_up(u, w_gate, w_up, start, cols, blk):
    rows, kdim = u.shape
    half = rows // 2
    first = start // blk
    shape = jax.ShapeDtypeStruct((2, half, cols), F32)
    wspec = pl.BlockSpec((kdim, blk), lambda i: (0, i + first))
    ospec = pl.BlockSpec((2, half, blk), lambda i: (0, 0, i))
    return pl.pallas_call(
        gu_kernel,
        grid=(cols // blk,),
        out_shape=[shape, shape],
        in_specs=[pl.BlockSpec((rows, kdim), lambda i: (0, 0)), wspec, wspec],
        out_specs=[ospec, ospec],
        compiler_params=pltpu.CompilerParams(vmem_limit_bytes=56 * 2**20),
        cost_estimate=pl.CostEstimate(
            flops=4 * rows * kdim * cols, bytes_accessed=4 * kdim * cols, transcendentals=0
        ),
        name="gate_up",
    )(u, w_gate, w_up)


def attn_kernel(nb, ahead, pos_ref, q_ref, kn_ref, vn_ref, cos_ref, sin_ref, kc_ref, vc_ref,
                o_ref, ko_ref, vo_ref, kbuf, vbuf, krow, vrow, ki, vi, ks, vs):
    n_seq, n_head, dim = q_ref.shape
    length = kbuf.shape[1]

    def fetch(b, slot):
        pltpu.make_async_copy(kc_ref.at[b], kbuf.at[slot], ki.at[slot]).start()
        pltpu.make_async_copy(vc_ref.at[b], vbuf.at[slot], vi.at[slot]).start()

    def wait_out(b, slot):
        pltpu.make_async_copy(kbuf.at[slot], ko_ref.at[b], ks.at[slot]).wait()
        pltpu.make_async_copy(vbuf.at[slot], vo_ref.at[b], vs.at[slot]).wait()

    for b in range(ahead):
        fetch(b, b)
    krow[...] = rope(kn_ref[...].astype(F32), cos_ref[...], sin_ref[...]).astype(BF16).astype(F32)
    vrow[...] = vn_ref[...].astype(F32)

    def patch(buf, slot, row, p):
        base = pl.multiple_of((p // 16) * 16, 16)
        old = buf[slot, pl.ds(base, 16), :].astype(F32)
        hit = lax.broadcasted_iota(jnp.int32, old.shape, 0) == p - base
        buf[slot, pl.ds(base, 16), :] = jnp.where(hit, row, old).astype(BF16)

    @pl.loop(0, n_seq // 2)
    def _(i):
        work = []
        for j in range(2):
            b = 2 * i + j
            slot = lax.rem(b, nb)
            nxt = b + ahead
            nslot = lax.rem(nxt, nb)

            @pl.when(jnp.logical_and(nxt < n_seq, nxt >= nb))
            def _():
                wait_out(nxt - nb, nslot)

            @pl.when(nxt < n_seq)
            def _():
                fetch(nxt, nslot)

            work.append((b, slot))
        for b, slot in work:
            p = pos_ref[b]
            pltpu.make_async_copy(kc_ref.at[b], kbuf.at[slot], ki.at[slot]).wait()
            patch(kbuf, slot, krow[pl.ds(b, 1), :], p)
            pltpu.make_async_copy(vc_ref.at[b], vbuf.at[slot], vi.at[slot]).wait()
            patch(vbuf, slot, vrow[pl.ds(b, 1), :], p)
        for b, slot in work:
            p = pos_ref[b]
            q = rope(q_ref[b].astype(F32), cos_ref[pl.ds(b, 1), :], sin_ref[pl.ds(b, 1), :]).astype(BF16)
            s = lax.dot_general(q, kbuf[slot], (((1,), (1,)), ((), ())), preferred_element_type=F32)
            s = s * (dim ** -0.5)
            ok = lax.broadcasted_iota(jnp.int32, (n_head, length), 1) <= p
            s = jnp.where(ok, s, -jnp.inf)
            e = jnp.exp(s - jnp.max(s, axis=1, keepdims=True))
            prob = (e / jnp.sum(e, axis=1, keepdims=True)).astype(BF16)
            o = jnp.dot(prob, vbuf[slot], preferred_element_type=F32)
            o_ref[b] = o.astype(BF16)
        for b, slot in work:
            pltpu.make_async_copy(kbuf.at[slot], ko_ref.at[b], ks.at[slot]).start()
            pltpu.make_async_copy(vbuf.at[slot], vo_ref.at[b], vs.at[slot]).start()

    for b in range(n_seq - nb, n_seq):
        wait_out(b, b % nb)


def attention(q, k_new, v_new, cos, sin, k_cache, v_cache, positions, nb=8, ahead=4):
    n_seq, length, dim = k_cache.shape
    n_head = q.shape[1]
    vm = pl.BlockSpec(memory_space=pltpu.VMEM)
    hbm = pl.BlockSpec(memory_space=pltpu.HBM)
    return pl.pallas_call(
        functools.partial(attn_kernel, nb, ahead),
        out_shape=[
            jax.ShapeDtypeStruct(q.shape, BF16),
            jax.ShapeDtypeStruct(k_cache.shape, BF16),
            jax.ShapeDtypeStruct(v_cache.shape, BF16),
        ],
        in_specs=[pl.BlockSpec(memory_space=pltpu.SMEM), vm, vm, vm, vm, vm, hbm, hbm],
        out_specs=[vm, hbm, hbm],
        scratch_shapes=[
            pltpu.VMEM((nb, length, dim), BF16),
            pltpu.VMEM((nb, length, dim), BF16),
            pltpu.VMEM((n_seq, dim), F32),
            pltpu.VMEM((n_seq, dim), F32),
            pltpu.SemaphoreType.DMA((nb,)),
            pltpu.SemaphoreType.DMA((nb,)),
            pltpu.SemaphoreType.DMA((nb,)),
            pltpu.SemaphoreType.DMA((nb,)),
        ],
        compiler_params=pltpu.CompilerParams(vmem_limit_bytes=56 * 2**20),
        cost_estimate=pl.CostEstimate(
            flops=4 * 10**10, bytes_accessed=8 * n_seq * length * dim, transcendentals=n_seq * n_head * length
        ),
        name="attention",
    )(positions, q, k_new, v_new, cos, sin, k_cache, v_cache)


def tail_kernel(n_gu, cuts, n_w, *refs):
    keeps, recvs = refs[:n_gu], refs[n_gu : 2 * n_gu]
    (o_ref, h_ref, wd_hbm, wo_hbm, out_ref, wd, kbuf, rbuf, aown, aoth, give, hold, got1, pass_, got2,
     wsem, ksem, rsem, as_, ar, s1, r1, s2, r2) = refs[2 * n_gu :]
    ix, iy = lax.axis_index("tpx"), lax.axis_index("tpy")
    half = aown.shape[0]
    gcols = kbuf.shape[3]
    width = h_ref.shape[1]
    kact, ko = wd_hbm.shape[0], wo_hbm.shape[0]
    partner = iy + 1 - 2 * lax.rem(iy, 2)
    cross = lax.rem(iy + 2, 4)
    core, chip = lax.rem(iy, 2), iy // 2
    peer_x = {"tpx": 1 - ix, "tpy": iy}
    peer_core = {"tpx": ix, "tpy": partner}
    peer_chip = {"tpx": ix, "tpy": cross}

    gu_loads = []
    for r, (r0, rn) in enumerate(cuts):
        group = []
        rows = pl.ds(r0, rn)
        for g in range(n_gu):
            group.append(pltpu.make_async_copy(keeps[g].at[:, rows], kbuf.at[g, :, rows], ksem.at[r, g]))
            group.append(pltpu.make_async_copy(recvs[g].at[:, rows], rbuf.at[g, :, rows], rsem.at[r, g]))
        for c in group:
            c.start()
        gu_loads.append(group)
    step = kact // n_w
    w_loads = []
    for j in range(n_w + 1):
        if j < n_w:
            src, dst = wd_hbm.at[pl.ds(j * step, step)], wd.at[pl.ds(j * step, step)]
        else:
            src, dst = wo_hbm, wd.at[pl.ds(kact, ko)]
        c = pltpu.make_async_copy(src, dst, wsem.at[j])
        c.start()
        w_loads.append(c)

    barrier = pltpu.get_barrier_semaphore()
    for d in (peer_x, peer_core, peer_chip):
        pl.semaphore_signal(barrier, inc=1, device_id=d, device_id_type=MESH)
    pl.semaphore_wait(barrier, 3)

    sends = []
    for r, (r0, rn) in enumerate(cuts):
        rows = pl.ds(r0, rn)
        for c in gu_loads[r]:
            c.wait()
        for g in range(n_gu):
            gate = (kbuf[g, 0, rows, :] + rbuf[g, 0, rows, :]).astype(BF16).astype(F32)
            up = (kbuf[g, 1, rows, :] + rbuf[g, 1, rows, :]).astype(BF16).astype(F32)
            aown[rows, g * gcols : (g + 1) * gcols] = (jax.nn.silu(gate) * up).astype(BF16)
        aown[rows, kact:] = o_ref[rows, :]
        c = pltpu.make_async_remote_copy(
            src_ref=aown.at[rows],
            dst_ref=aoth.at[rows],
            send_sem=as_.at[r],
            recv_sem=ar.at[r],
            device_id=peer_x,
            device_id_type=MESH,
        )
        c.start()
        sends.append(c)
    for c in w_loads:
        c.wait()

    blocks = [(half, half)] + [(r0, rn) for r0, rn in cuts]

    def product(lhs, x, c):
        col = pl.ds(pl.multiple_of((x * 2 + c) * width, width), width)
        return jnp.dot(lhs, wd[:, col], preferred_element_type=F32)

    stage1, stage2 = [], []

    def run_block(k):
        r0, rn = blocks[k]
        rows = pl.ds(r0, rn)
        if k == 0:
            lhs = aown[...]
        else:
            sends[k - 1].wait_recv()
            lhs = aoth[rows, :]
        for x in range(2):
            give[x, rows, :] = product(lhs, x, 1 - core)
        c = pltpu.make_async_remote_copy(
            src_ref=give.at[:, rows],
            dst_ref=got1.at[:, rows],
            send_sem=s1.at[k],
            recv_sem=r1.at[k],
            device_id=peer_core,
            device_id_type=MESH,
        )
        c.start()
        stage1.append(c)
        hold[0, rows, :] = product(lhs, 1 - chip, core)
        hold[1, rows, :] = product(lhs, chip, core)

    def reduce_block(k):
        r0, rn = blocks[k]
        rows = pl.ds(r0, rn)
        stage1[k].wait_recv()
        pass_[rows, :] = hold[0, rows, :] + got1[1 - chip, rows, :]
        c = pltpu.make_async_remote_copy(
            src_ref=pass_.at[rows],
            dst_ref=got2.at[rows],
            send_sem=s2.at[k],
            recv_sem=r2.at[k],
            device_id=peer_chip,
            device_id_type=MESH,
        )
        c.start()
        stage2.append(c)

    def finish_block(k):
        r0, rn = blocks[k]
        rows = pl.ds(r0, rn)
        stage2[k].wait_recv()
        total = hold[1, rows, :] + got1[chip, rows, :] + got2[rows, :]
        base = ix * half if k == 0 else (1 - ix) * half + r0
        nat = pl.ds(pl.multiple_of(base, 32), rn)
        out_ref[nat, :] = (h_ref[nat, :].astype(F32) + total).astype(BF16)

    n_blk = len(blocks)
    for k in range(n_blk):
        run_block(k)
        if k:
            reduce_block(k - 1)
    reduce_block(n_blk - 1)
    for k in range(n_blk):
        finish_block(k)
    for c in sends + stage1 + stage2:
        c.wait_send()


def tail(keeps, recvs, o_own, hidden, w_down, w_o):
    rows, width = hidden.shape
    n_gu = len(keeps)
    _, half, gcols = keeps[0].shape
    n = w_down.shape[1]
    kdim = w_down.shape[0] + w_o.shape[0]
    cuts = [(0, 64), (64, 32), (96, 32)]
    n_w, n_cut, n_blk = 8, len(cuts), len(cuts) + 1
    vm = pl.BlockSpec(memory_space=pltpu.VMEM)
    anywhere = pl.BlockSpec(memory_space=pl.ANY)
    dma = pltpu.SemaphoreType.DMA
    return pl.pallas_call(
        functools.partial(tail_kernel, n_gu, cuts, n_w),
        out_shape=jax.ShapeDtypeStruct((rows, width), BF16),
        in_specs=[anywhere] * (2 * n_gu) + [vm, vm] + [pl.BlockSpec(memory_space=pltpu.HBM)] * 2,
        out_specs=vm,
        scratch_shapes=[
            pltpu.VMEM((kdim, n), BF16),
            pltpu.VMEM((n_gu, 2, half, gcols), F32),
            pltpu.VMEM((n_gu, 2, half, gcols), F32),
            pltpu.VMEM((half, kdim), BF16),
            pltpu.VMEM((half, kdim), BF16),
            pltpu.VMEM((2, rows, width), F32),
            pltpu.VMEM((2, rows, width), F32),
            pltpu.VMEM((2, rows, width), F32),
            pltpu.VMEM((rows, width), F32),
            pltpu.VMEM((rows, width), F32),
            dma((n_w + 1,)),
            dma((n_cut, n_gu)),
            dma((n_cut, n_gu)),
            dma((n_cut,)),
            dma((n_cut,)),
            dma((n_blk,)),
            dma((n_blk,)),
            dma((n_blk,)),
            dma((n_blk,)),
        ],
        compiler_params=pltpu.CompilerParams(collective_id=1, has_side_effects=True, vmem_limit_bytes=56 * 2**20),
        cost_estimate=pl.CostEstimate(flops=2 * rows * kdim * n, bytes_accessed=2 * kdim * n, transcendentals=0),
        name="tail",
    )(*keeps, *recvs, o_own, hidden, w_down, w_o)


def solution(mesh):
    x_size = mesh.shape["tpx"]
    y_size = mesh.shape["tpy"]
    hidden_spec = P("dp", ("tpx", "tpy"))
    cache_spec = P(("dp", "tpx", "tpy"), None, None)
    in_specs = (hidden_spec, P(("tpx", "tpy")), P("tpx", "tpy"), P("tpx", None), P("tpx", None), P("tpx", "tpy"), P("tpx", "tpy"), P("tpy", "tpx"), P("tpy", "tpx"), cache_spec, cache_spec, P(("dp", "tpx", "tpy")))
    out_specs = (hidden_spec, cache_spec, cache_spec)
    swap_x = [(0, 1), (1, 0)]
    n_chunk = 4

    def device_step(hidden, ln_scale, w_q, w_k, w_v, w_gate, w_up, w_o, w_down, k_cache, v_cache, positions):
        iy = lax.axis_index("tpy")
        rows, _ = hidden.shape
        half = rows // 2
        n_seq = positions.shape[0]
        dim = k_cache.shape[2]
        cols = w_gate.shape[1]

        def dot(a, b):
            return jnp.dot(a, b, preferred_element_type=F32)

        u = front(x_size, y_size, hidden, ln_scale)
        u_oth, u_own = u[:half], u[half:]
        q_send = dot(u_oth, w_q)
        kv_rows_oth = lax.dynamic_slice_in_dim(u_oth, iy * n_seq, n_seq, axis=0)
        kv_rows_own = lax.dynamic_slice_in_dim(u_own, iy * n_seq, n_seq, axis=0)
        kv_send = jnp.concatenate([dot(kv_rows_oth, w_k), dot(kv_rows_oth, w_v)], axis=1)
        q_recv = lax.ppermute(q_send, "tpx", swap_x)
        kv_recv = lax.ppermute(kv_send, "tpx", swap_x)

        per = cols // n_chunk
        keep, recv = [], []
        for c in range(n_chunk):
            s, k = gate_up(u, w_gate, w_up, c * per, per, 512)
            keep.append(k)
            recv.append(lax.ppermute(s, "tpx", swap_x))

        q_own = dot(u_own, w_q)
        kv_own = jnp.concatenate([dot(kv_rows_own, w_k), dot(kv_rows_own, w_v)], axis=1)
        q_heads = (q_own + q_recv).astype(BF16).reshape(half, -1, dim)
        kv_new = (kv_own + kv_recv).astype(BF16)
        q_seq = lax.all_to_all(q_heads, "tpy", 0, 1, tiled=True)
        cos_tab, sin_tab = rope_tables(positions, dim)
        attn_seq, k_all, v_all = attention(q_seq, kv_new[:, :dim], kv_new[:, dim:], cos_tab, sin_tab, k_cache, v_cache, positions)

        attn_heads = lax.all_to_all(attn_seq, "tpy", 1, 0, tiled=True)
        o_own = attn_heads.reshape(half, -1)
        hidden_out = tail(keep, recv, o_own, hidden, w_down, w_o)
        return hidden_out, k_all, v_all

    return jax.shard_map(device_step, mesh=mesh, in_specs=in_specs, out_specs=out_specs, check_vma=False)
```

```python
import functools

import jax
import jax.numpy as jnp
from jax import lax
from jax.experimental import pallas as pl
from jax.experimental.pallas import tpu as pltpu
from jax.sharding import PartitionSpec as P


LN_EPS = 1e-6
ROPE_BASE = 10000.0
MESH = pl.DeviceIdType.MESH
F32 = jnp.float32
BF16 = jnp.bfloat16


def rope_tables(positions, head_dim):
    half_dim = head_dim // 2
    inv_freq = ROPE_BASE ** (-(jnp.arange(half_dim, dtype=F32) * 2.0 / head_dim))
    angles = positions.astype(F32)[:, None] * inv_freq[None, :]
    return jnp.cos(angles), jnp.sin(angles)


def rope(x, cos, sin):
    half = x.shape[-1] // 2
    lead, tail = x[:, :half], x[:, half:]
    return jnp.concatenate([lead * cos - tail * sin, lead * sin + tail * cos], axis=-1)


def front_kernel(nx, ny, ge, gc, h_ref, sc_ref, wq_hbm, wk_hbm, wv_hbm, wg_hbm, wu_hbm,
                 q_ref, kv_ref, ke_ref, re_ref, u_hbm, gs_hbm, gk_hbm,
                 hbuf, scbuf, stat, cols, u_ref, wq, wkv, wgu, qs, qr, qo, kvs, kvr, es, er, gs, gk, qn, qall,
                 wsem, hs, hr, ss, sr, ts, tr, qss, qrs, ls, as_, ar, outs):
    ix, iy = lax.axis_index("tpx"), lax.axis_index("tpy")
    rows, width = h_ref.shape
    n_dev = nx * ny
    half = rows // 2
    n_seq = half // ny
    dim = wk_hbm.shape[1]
    gw = ge + gc
    partner = iy + 1 - 2 * lax.rem(iy, 2)
    cross = lax.rem(iy + 2, ny)
    diag = lax.rem(partner + 2, ny)
    me = ix * ny + iy
    peer_x = {"tpx": 1 - ix, "tpy": iy}

    def remote(src, dst, send, recv, dev):
        return pltpu.make_async_remote_copy(
            src_ref=src, dst_ref=dst, send_sem=send, recv_sem=recv, device_id=dev, device_id_type=MESH
        )

    loads = [
        pltpu.make_async_copy(wq_hbm, wq, wsem.at[0]),
        pltpu.make_async_copy(wk_hbm, wkv.at[0], wsem.at[1]),
        pltpu.make_async_copy(wv_hbm, wkv.at[1], wsem.at[2]),
        pltpu.make_async_copy(wg_hbm.at[:, 0:gw], wgu.at[0], wsem.at[3]),
        pltpu.make_async_copy(wu_hbm.at[:, 0:gw], wgu.at[1], wsem.at[4]),
    ]
    for c in loads:
        c.start()

    others = [(dx, dy) for dx in range(nx) for dy in range(ny) if dx or dy]
    barrier = pltpu.get_barrier_semaphore()
    for dx, dy in others:
        pl.semaphore_signal(
            barrier,
            inc=1,
            device_id={"tpx": lax.rem(ix + dx, nx), "tpy": lax.rem(iy + dy, ny)},
            device_id_type=MESH,
        )
    pl.semaphore_wait(barrier, n_dev - 1)

    n_ch, ch = 4, rows // 4

    def nat(j):
        base = (1 - ix) * half + j * ch if j < n_ch // 2 else ix * half + (j - n_ch // 2) * ch
        return pl.ds(pl.multiple_of(base, ch), ch)

    def perm(j):
        return pl.ds(j * ch, ch)

    def h_copy(j, dst_y, k):
        return remote(h_ref.at[nat(j)], hbuf.at[iy, perm(j)], hs.at[k, j], hr.at[k, j], {"tpx": ix, "tpy": dst_y})

    to_cross = [h_copy(j, cross, 0) for j in range(n_ch)]
    to_partner = [h_copy(j, partner, 1) for j in range(n_ch)]
    to_cross[0].start()
    for c in to_partner:
        c.start()

    hf = h_ref[...].astype(F32)
    total = jnp.sum(hf, axis=1, keepdims=True)
    dev = hf - total / width
    spread = jnp.sum(dev * dev, axis=1, keepdims=True)
    lane = lax.broadcasted_iota(jnp.int32, (rows, 128), 1)
    packed = jnp.where(lane == 0, total, jnp.where(lane == 1, spread, 0.0))
    stat[me] = jnp.transpose(packed)[:2]
    stat_copies = []
    for k, (dx, dy) in enumerate(others):
        c = remote(
            stat.at[me], stat.at[me], ts.at[k], tr.at[k],
            {"tpx": lax.rem(ix + dx, nx), "tpy": lax.rem(iy + dy, ny)},
        )
        c.start()
        stat_copies.append(c)
    sc_copies = []
    for k, dst in enumerate((cross, partner, diag)):
        c = remote(sc_ref, scbuf.at[iy], ss.at[k], sr.at[k], {"tpx": ix, "tpy": dst})
        c.start()
        sc_copies.append(c)
    for c in to_cross[1:]:
        c.start()

    forward = []

    def relay(j):
        to_cross[j].wait_recv()
        part = hbuf.at[cross, perm(j)]
        c = remote(part, part, hs.at[2, j], hr.at[2, j], {"tpx": ix, "tpy": partner})
        c.start()
        forward.append(c)

    relay(0)
    for c in stat_copies:
        c.wait_recv()
    sums = [stat[d, 0:1, :] for d in range(n_dev)]
    sprd = [stat[d, 1:2, :] for d in range(n_dev)]
    mean = functools.reduce(jnp.add, sums) / (width * n_dev)
    m2 = functools.reduce(jnp.add, sprd)
    for d in range(n_dev):
        gap = sums[d] / width - mean
        m2 = m2 + width * gap * gap
    rs = lax.rsqrt(m2 / (width * n_dev) + LN_EPS)
    sub = lax.broadcasted_iota(jnp.int32, (128, rows), 0)
    cols[...] = jnp.transpose(jnp.where(sub == 0, mean, jnp.where(sub == 1, rs, 0.0)))
    for c in sc_copies:
        c.wait_recv()

    def emit(block, scale, owner, j):
        stats = cols[nat(j), :]
        u = ((block.astype(F32) - stats[:, 0:1]) * stats[:, 1:2] * scale).astype(BF16)
        u_ref[perm(j), pl.ds(pl.multiple_of(owner * width, width), width)] = u

    def normalise(j):
        emit(h_ref[nat(j), :], sc_ref[...], iy, j)
        to_partner[j].wait_recv()
        emit(hbuf[partner, perm(j), :], scbuf[partner], partner, j)
        emit(hbuf[cross, perm(j), :], scbuf[cross], cross, j)
        forward[j].wait_recv()
        emit(hbuf[diag, perm(j), :], scbuf[diag], diag, j)

    def dot(a, b):
        return jnp.dot(a, b, preferred_element_type=F32)

    q_copies = []
    for j in range(n_ch):
        if j + 1 < n_ch:
            relay(j + 1)
        normalise(j)
        if j < n_ch // 2:
            if j == 0:
                loads[0].wait()
            qs[perm(j), :] = dot(u_ref[perm(j), :], wq[...])
            c = remote(qs.at[perm(j)], qr.at[perm(j)], qss.at[j], qrs.at[j], peer_x)
            c.start()
            q_copies.append(c)
    loads[1].wait()
    loads[2].wait()
    oth_rows = u_ref[pl.ds(pl.multiple_of(iy * n_seq, n_seq), n_seq), :]
    own_rows = u_ref[pl.ds(pl.multiple_of(half + iy * n_seq, n_seq), n_seq), :]
    for k in range(2):
        kvs[:, k * dim : (k + 1) * dim] = dot(oth_rows, wkv[k])
    kv_copy = remote(kvs, kvr, ls.at[0], ls.at[1], peer_x)
    kv_copy.start()
    u_out = pltpu.make_async_copy(u_ref, u_hbm, outs.at[0])
    u_out.start()
    loads[3].wait()
    loads[4].wait()
    for k in range(2):
        y = dot(u_ref[...], wgu[k, :, 0:ge])
        es[k] = y[:half]
        ke_ref[k] = y[half:]
    e_copy = remote(es, er, ls.at[2], ls.at[3], peer_x)
    e_copy.start()
    qo[...] = dot(u_ref[pl.ds(half, half), :], wq[...])
    own_kv = [dot(own_rows, wkv[k]) for k in range(2)]

    def gate_up_part(lo, hi):
        for k in range(2):
            y = dot(u_ref[...], wgu[k, :, ge + lo : ge + hi])
            gs[k, :, lo:hi] = y[:half]
            gk[k, :, lo:hi] = y[half:]

    gate_up_part(0, gc // 2)
    for j in range(n_ch // 2):
        q_copies[j].wait_recv()
        qn[perm(j), :] = (qo[perm(j), :] + qr[perm(j), :]).astype(BF16)
    q_sends = []
    for k in range(1, ny):
        d = lax.rem(iy + k, ny)
        c = remote(
            qn.at[pl.ds(pl.multiple_of(d * n_seq, n_seq), n_seq)], qall.at[iy],
            as_.at[k - 1], ar.at[k - 1], {"tpx": ix, "tpy": d},
        )
        c.start()
        q_sends.append(c)
    gate_up_part(gc // 2, gc)
    g_out = [pltpu.make_async_copy(gs, gs_hbm, outs.at[1]), pltpu.make_async_copy(gk, gk_hbm, outs.at[2])]
    for c in g_out:
        c.start()
    kv_copy.wait_recv()
    for k in range(2):
        sl = slice(k * dim, (k + 1) * dim)
        kv_ref[:, sl] = (own_kv[k] + kvr[:, sl]).astype(BF16)
    q_ref[iy] = qn[pl.ds(pl.multiple_of(iy * n_seq, n_seq), n_seq), :].astype(F32)
    for k in range(1, ny):
        q_sends[k - 1].wait_recv()
        src = lax.rem(iy + ny - k, ny)
        q_ref[src] = qall[src].astype(F32)
    e_copy.wait_recv()
    re_ref[...] = er[...]
    for c in to_cross + to_partner + forward + sc_copies + stat_copies + q_copies + q_sends + [kv_copy, e_copy]:
        c.wait_send()
    for c in [u_out] + g_out:
        c.wait()


def front(nx, ny, ge, gc, hidden, ln_scale, w_q, w_k, w_v, w_gate, w_up):
    rows, width = hidden.shape
    half = rows // 2
    n_dev, n_seq = nx * ny, rows // (nx * ny)
    kdim, nq = w_q.shape
    dim = w_k.shape[1]
    vm = pl.BlockSpec(memory_space=pltpu.VMEM)
    hbm = pl.BlockSpec(memory_space=pltpu.HBM)
    dma = pltpu.SemaphoreType.DMA
    sds = jax.ShapeDtypeStruct
    return pl.pallas_call(
        functools.partial(front_kernel, nx, ny, ge, gc),
        out_shape=[
            sds((ny, n_seq, nq), F32),
            sds((n_seq, 2 * dim), BF16),
            sds((2, half, ge), F32),
            sds((2, half, ge), F32),
            sds((rows, kdim), BF16),
            sds((2, half, gc), F32),
            sds((2, half, gc), F32),
        ],
        in_specs=[vm, vm] + [hbm] * 5,
        out_specs=[vm] * 4 + [hbm] * 3,
        scratch_shapes=[
            pltpu.VMEM((ny, rows, width), BF16),
            pltpu.VMEM((ny, 1, width), F32),
            pltpu.VMEM((n_dev, 2, rows), F32),
            pltpu.VMEM((rows, 128), F32),
            pltpu.VMEM((rows, kdim), BF16),
            pltpu.VMEM((kdim, nq), BF16),
            pltpu.VMEM((2, kdim, dim), BF16),
            pltpu.VMEM((2, kdim, ge + gc), BF16),
            pltpu.VMEM((half, nq), F32),
            pltpu.VMEM((half, nq), F32),
            pltpu.VMEM((half, nq), F32),
            pltpu.VMEM((n_seq, 2 * dim), F32),
            pltpu.VMEM((n_seq, 2 * dim), F32),
            pltpu.VMEM((2, half, ge), F32),
            pltpu.VMEM((2, half, ge), F32),
            pltpu.VMEM((2, half, gc), F32),
            pltpu.VMEM((2, half, gc), F32),
            pltpu.VMEM((half, nq), BF16),
            pltpu.VMEM((ny, n_seq, nq), BF16),
            dma((5,)),
            dma((3, 4)),
            dma((3, 4)),
            dma((3,)),
            dma((3,)),
            dma((n_dev - 1,)),
            dma((n_dev - 1,)),
            dma((2,)),
            dma((2,)),
            dma((4,)),
            dma((ny - 1,)),
            dma((ny - 1,)),
            dma((3,)),
        ],
        compiler_params=pltpu.CompilerParams(collective_id=0, has_side_effects=True, vmem_limit_bytes=56 * 2**20),
        cost_estimate=pl.CostEstimate(flops=2 * rows * kdim * nq, bytes_accessed=2 * kdim * nq, transcendentals=0),
        name="front",
    )(hidden, ln_scale.reshape(1, width), w_q, w_k, w_v, w_gate, w_up)


def gu_kernel(u_ref, wg_ref, wu_ref, send, keep):
    half = u_ref.shape[0] // 2
    for k, w_ref in enumerate((wg_ref, wu_ref)):
        y = jnp.dot(u_ref[...], w_ref[...], preferred_element_type=F32)
        send[k] = y[:half]
        keep[k] = y[half:]


def gate_up(u, w_gate, w_up, start, cols, blk):
    rows, kdim = u.shape
    half = rows // 2
    first = start // blk
    shape = jax.ShapeDtypeStruct((2, half, cols), F32)
    wspec = pl.BlockSpec((kdim, blk), lambda i: (0, i + first))
    ospec = pl.BlockSpec((2, half, blk), lambda i: (0, 0, i))
    return pl.pallas_call(
        gu_kernel,
        grid=(cols // blk,),
        out_shape=[shape, shape],
        in_specs=[pl.BlockSpec((rows, kdim), lambda i: (0, 0)), wspec, wspec],
        out_specs=[ospec, ospec],
        compiler_params=pltpu.CompilerParams(vmem_limit_bytes=56 * 2**20),
        cost_estimate=pl.CostEstimate(
            flops=4 * rows * kdim * cols, bytes_accessed=4 * kdim * cols, transcendentals=0
        ),
        name="gate_up",
    )(u, w_gate, w_up)


def attn_kernel(nb, ahead, pos_ref, q_ref, kv_ref, cos_ref, sin_ref, kc_ref, vc_ref,
                o_ref, ko_ref, vo_ref, kbuf, vbuf, krow, vrow, qrot, orow, ki, vi, ks, vs):
    n_seq, n_head, dim = qrot.shape
    n_dev = q_ref.shape[0]
    per = n_head // n_dev
    length = kbuf.shape[1]

    def fetch(b, slot):
        pltpu.make_async_copy(kc_ref.at[b], kbuf.at[slot], ki.at[slot]).start()
        pltpu.make_async_copy(vc_ref.at[b], vbuf.at[slot], vi.at[slot]).start()

    def wait_out(b, slot):
        pltpu.make_async_copy(kbuf.at[slot], ko_ref.at[b], ks.at[slot]).wait()
        pltpu.make_async_copy(vbuf.at[slot], vo_ref.at[b], vs.at[slot]).wait()

    for b in range(ahead):
        fetch(b, b)
    krow[...] = rope(kv_ref[:, :dim].astype(F32), cos_ref[...], sin_ref[...]).astype(BF16).astype(F32)
    vrow[...] = kv_ref[:, dim:].astype(F32)
    for d in range(n_dev):
        for h in range(per):
            x = rope(q_ref[d, :, h * dim : (h + 1) * dim], cos_ref[...], sin_ref[...])
            qrot[:, d * per + h, :] = x

    def patch(buf, slot, row, p):
        base = pl.multiple_of((p // 16) * 16, 16)
        old = buf[slot, pl.ds(base, 16), :].astype(F32)
        hit = lax.broadcasted_iota(jnp.int32, old.shape, 0) == p - base
        buf[slot, pl.ds(base, 16), :] = jnp.where(hit, row, old).astype(BF16)

    @pl.loop(0, n_seq // 2)
    def _(i):
        work = []
        for j in range(2):
            b = 2 * i + j
            slot = lax.rem(b, nb)
            nxt = b + ahead
            nslot = lax.rem(nxt, nb)

            @pl.when(jnp.logical_and(nxt < n_seq, nxt >= nb))
            def _():
                wait_out(nxt - nb, nslot)

            @pl.when(nxt < n_seq)
            def _():
                fetch(nxt, nslot)

            work.append((b, slot))
        for b, slot in work:
            p = pos_ref[b]
            pltpu.make_async_copy(kc_ref.at[b], kbuf.at[slot], ki.at[slot]).wait()
            patch(kbuf, slot, krow[pl.ds(b, 1), :], p)
            pltpu.make_async_copy(vc_ref.at[b], vbuf.at[slot], vi.at[slot]).wait()
            patch(vbuf, slot, vrow[pl.ds(b, 1), :], p)
        for b, slot in work:
            p = pos_ref[b]
            q = qrot[b].astype(BF16)
            s = lax.dot_general(q, kbuf[slot], (((1,), (1,)), ((), ())), preferred_element_type=F32)
            s = s * (dim ** -0.5)
            ok = lax.broadcasted_iota(jnp.int32, (n_head, length), 1) <= p
            s = jnp.where(ok, s, -jnp.inf)
            e = jnp.exp(s - jnp.max(s, axis=1, keepdims=True))
            prob = (e / jnp.sum(e, axis=1, keepdims=True)).astype(BF16)
            o = jnp.dot(prob, vbuf[slot], preferred_element_type=F32)
            for h in range(n_head):
                orow[h // per, pl.ds(b, 1), (h % per) * dim : (h % per + 1) * dim] = o[h : h + 1]
        for b, slot in work:
            pltpu.make_async_copy(kbuf.at[slot], ko_ref.at[b], ks.at[slot]).start()
            pltpu.make_async_copy(vbuf.at[slot], vo_ref.at[b], vs.at[slot]).start()

    o_ref[...] = orow[...].astype(BF16)
    for b in range(n_seq - nb, n_seq):
        wait_out(b, b % nb)


def attention(q, kv_new, cos, sin, k_cache, v_cache, positions, nb=8, ahead=4):
    n_seq, length, dim = k_cache.shape
    n_head = q.shape[0] * q.shape[2] // dim
    vm = pl.BlockSpec(memory_space=pltpu.VMEM)
    hbm = pl.BlockSpec(memory_space=pltpu.HBM)
    return pl.pallas_call(
        functools.partial(attn_kernel, nb, ahead),
        out_shape=[
            jax.ShapeDtypeStruct(q.shape, BF16),
            jax.ShapeDtypeStruct(k_cache.shape, BF16),
            jax.ShapeDtypeStruct(v_cache.shape, BF16),
        ],
        in_specs=[pl.BlockSpec(memory_space=pltpu.SMEM), vm, vm, vm, vm, hbm, hbm],
        out_specs=[vm, hbm, hbm],
        scratch_shapes=[
            pltpu.VMEM((nb, length, dim), BF16),
            pltpu.VMEM((nb, length, dim), BF16),
            pltpu.VMEM((n_seq, dim), F32),
            pltpu.VMEM((n_seq, dim), F32),
            pltpu.VMEM((n_seq, n_head, dim), F32),
            pltpu.VMEM(q.shape, F32),
            pltpu.SemaphoreType.DMA((nb,)),
            pltpu.SemaphoreType.DMA((nb,)),
            pltpu.SemaphoreType.DMA((nb,)),
            pltpu.SemaphoreType.DMA((nb,)),
        ],
        compiler_params=pltpu.CompilerParams(vmem_limit_bytes=56 * 2**20),
        cost_estimate=pl.CostEstimate(
            flops=4 * 10**10, bytes_accessed=8 * n_seq * length * dim, transcendentals=n_seq * n_head * length
        ),
        name="attention",
    )(positions, q, kv_new, cos, sin, k_cache, v_cache)


def tail_kernel(n_gu, cuts, n_w, *refs):
    keeps, recvs = refs[:n_gu], refs[n_gu : 2 * n_gu]
    (o_ref, h_ref, wd_hbm, wo_hbm, out_ref, wd, kbuf, rbuf, aown, aoth, give, hold, got1, pass_, got2,
     wsem, ksem, rsem, as_, ar, s1, r1, s2, r2, os_, or_) = refs[2 * n_gu :]
    ix, iy = lax.axis_index("tpx"), lax.axis_index("tpy")
    half = aown.shape[0]
    ny, n_seq = o_ref.shape[0], o_ref.shape[1]
    starts, at = [], 0
    for ref in keeps:
        starts.append((at, ref.shape[2]))
        at += ref.shape[2]
    width = h_ref.shape[1]
    kact, ko = wd_hbm.shape[0], wo_hbm.shape[0]
    partner = iy + 1 - 2 * lax.rem(iy, 2)
    cross = lax.rem(iy + 2, 4)
    core, chip = lax.rem(iy, 2), iy // 2
    peer_x = {"tpx": 1 - ix, "tpy": iy}
    peer_core = {"tpx": ix, "tpy": partner}
    peer_chip = {"tpx": ix, "tpy": cross}

    gu_loads = []
    for r, (r0, rn) in enumerate(cuts):
        group = []
        rows = pl.ds(r0, rn)
        for g in range(n_gu):
            part = pl.ds(*starts[g])
            group.append(pltpu.make_async_copy(keeps[g].at[:, rows], kbuf.at[:, rows, part], ksem.at[r, g]))
            group.append(pltpu.make_async_copy(recvs[g].at[:, rows], rbuf.at[:, rows, part], rsem.at[r, g]))
        for c in group:
            c.start()
        gu_loads.append(group)
    step = kact // n_w
    w_loads = []
    for j in range(n_w + 1):
        if j < n_w:
            src, dst = wd_hbm.at[pl.ds(j * step, step)], wd.at[pl.ds(j * step, step)]
        else:
            src, dst = wo_hbm, wd.at[pl.ds(kact, ko)]
        c = pltpu.make_async_copy(src, dst, wsem.at[j])
        c.start()
        w_loads.append(c)

    barrier = pltpu.get_barrier_semaphore()
    others = [(dx, dy) for dx in (1, 0) for dy in range(ny) if dx or dy]

    def shifted(dx, dy):
        return {"tpx": lax.rem(ix + dx, 2), "tpy": lax.rem(iy + dy, ny)}

    for dx, dy in others:
        pl.semaphore_signal(barrier, inc=1, device_id=shifted(dx, dy), device_id_type=MESH)
    pl.semaphore_wait(barrier, len(others))

    o_rows = pl.ds(pl.multiple_of(iy * n_seq, n_seq), n_seq)
    o_cols = pl.ds(kact, ko)
    o_copies = []
    for k, (dx, dy) in enumerate(others):
        c = pltpu.make_async_remote_copy(
            src_ref=o_ref.at[lax.rem(iy + dy, ny)],
            dst_ref=(aoth if dx else aown).at[o_rows, o_cols],
            send_sem=os_.at[k],
            recv_sem=or_.at[k],
            device_id=shifted(dx, dy),
            device_id_type=MESH,
        )
        c.start()
        o_copies.append(c)
    aown[o_rows, kact:] = o_ref[iy]

    sends = []
    for r, (r0, rn) in enumerate(cuts):
        rows = pl.ds(r0, rn)
        for c in gu_loads[r]:
            c.wait()
        for g in range(n_gu):
            part = pl.ds(*starts[g])
            gate = (kbuf[0, rows, part] + rbuf[0, rows, part]).astype(BF16).astype(F32)
            up = (kbuf[1, rows, part] + rbuf[1, rows, part]).astype(BF16).astype(F32)
            aown[rows, part] = (jax.nn.silu(gate) * up).astype(BF16)
        c = pltpu.make_async_remote_copy(
            src_ref=aown.at[rows, pl.ds(0, kact)],
            dst_ref=aoth.at[rows, pl.ds(0, kact)],
            send_sem=as_.at[r],
            recv_sem=ar.at[r],
            device_id=peer_x,
            device_id_type=MESH,
        )
        c.start()
        sends.append(c)
    for c in w_loads:
        c.wait()
    for c in o_copies:
        c.wait_recv()

    blocks = [(half, half)] + [(r0, rn) for r0, rn in cuts]

    def product(lhs, x, c):
        col = pl.ds(pl.multiple_of((x * 2 + c) * width, width), width)
        return jnp.dot(lhs, wd[:, col], preferred_element_type=F32)

    stage1, stage2 = [], []

    def run_block(k):
        r0, rn = blocks[k]
        rows = pl.ds(r0, rn)
        if k == 0:
            lhs = aown[...]
        else:
            sends[k - 1].wait_recv()
            lhs = aoth[rows, :]
        for x in range(2):
            give[x, rows, :] = product(lhs, x, 1 - core)
        c = pltpu.make_async_remote_copy(
            src_ref=give.at[:, rows],
            dst_ref=got1.at[:, rows],
            send_sem=s1.at[k],
            recv_sem=r1.at[k],
            device_id=peer_core,
            device_id_type=MESH,
        )
        c.start()
        stage1.append(c)
        hold[0, rows, :] = product(lhs, 1 - chip, core)
        hold[1, rows, :] = product(lhs, chip, core)

    def reduce_block(k):
        r0, rn = blocks[k]
        rows = pl.ds(r0, rn)
        stage1[k].wait_recv()
        pass_[rows, :] = hold[0, rows, :] + got1[1 - chip, rows, :]
        c = pltpu.make_async_remote_copy(
            src_ref=pass_.at[rows],
            dst_ref=got2.at[rows],
            send_sem=s2.at[k],
            recv_sem=r2.at[k],
            device_id=peer_chip,
            device_id_type=MESH,
        )
        c.start()
        stage2.append(c)

    def finish_block(k):
        r0, rn = blocks[k]
        rows = pl.ds(r0, rn)
        stage2[k].wait_recv()
        total = hold[1, rows, :] + got1[chip, rows, :] + got2[rows, :]
        base = ix * half if k == 0 else (1 - ix) * half + r0
        nat = pl.ds(pl.multiple_of(base, 32), rn)
        out_ref[nat, :] = (h_ref[nat, :].astype(F32) + total).astype(BF16)

    n_blk = len(blocks)
    for k in range(n_blk):
        run_block(k)
        if k:
            reduce_block(k - 1)
    reduce_block(n_blk - 1)
    for k in range(n_blk):
        finish_block(k)
    for c in sends + stage1 + stage2 + o_copies:
        c.wait_send()


def tail(keeps, recvs, o, hidden, w_down, w_o):
    rows, width = hidden.shape
    n_gu = len(keeps)
    half = keeps[0].shape[1]
    n = w_down.shape[1]
    kdim = w_down.shape[0] + w_o.shape[0]
    cuts = [(0, 64), (64, 32), (96, 32)]
    n_w, n_cut, n_blk = 8, len(cuts), len(cuts) + 1
    vm = pl.BlockSpec(memory_space=pltpu.VMEM)
    anywhere = pl.BlockSpec(memory_space=pl.ANY)
    dma = pltpu.SemaphoreType.DMA
    return pl.pallas_call(
        functools.partial(tail_kernel, n_gu, cuts, n_w),
        out_shape=jax.ShapeDtypeStruct((rows, width), BF16),
        in_specs=[anywhere] * (2 * n_gu) + [vm, vm] + [pl.BlockSpec(memory_space=pltpu.HBM)] * 2,
        out_specs=vm,
        scratch_shapes=[
            pltpu.VMEM((kdim, n), BF16),
            pltpu.VMEM((2, half, w_down.shape[0]), F32),
            pltpu.VMEM((2, half, w_down.shape[0]), F32),
            pltpu.VMEM((half, kdim), BF16),
            pltpu.VMEM((half, kdim), BF16),
            pltpu.VMEM((2, rows, width), F32),
            pltpu.VMEM((2, rows, width), F32),
            pltpu.VMEM((2, rows, width), F32),
            pltpu.VMEM((rows, width), F32),
            pltpu.VMEM((rows, width), F32),
            dma((n_w + 1,)),
            dma((n_cut, n_gu)),
            dma((n_cut, n_gu)),
            dma((n_cut,)),
            dma((n_cut,)),
            dma((n_blk,)),
            dma((n_blk,)),
            dma((n_blk,)),
            dma((n_blk,)),
            dma((7,)),
            dma((7,)),
        ],
        compiler_params=pltpu.CompilerParams(collective_id=1, has_side_effects=True, vmem_limit_bytes=56 * 2**20),
        cost_estimate=pl.CostEstimate(flops=2 * rows * kdim * n, bytes_accessed=2 * kdim * n, transcendentals=0),
        name="tail",
    )(*keeps, *recvs, o, hidden, w_down, w_o)


def solution(mesh):
    x_size = mesh.shape["tpx"]
    y_size = mesh.shape["tpy"]
    hidden_spec = P("dp", ("tpx", "tpy"))
    cache_spec = P(("dp", "tpx", "tpy"), None, None)
    in_specs = (hidden_spec, P(("tpx", "tpy")), P("tpx", "tpy"), P("tpx", None), P("tpx", None), P("tpx", "tpy"), P("tpx", "tpy"), P("tpy", "tpx"), P("tpy", "tpx"), cache_spec, cache_spec, P(("dp", "tpx", "tpy")))
    out_specs = (hidden_spec, cache_spec, cache_spec)
    swap_x = [(0, 1), (1, 0)]
    ge, sizes = 256, (1024, 1024, 1024, 768)

    def device_step(hidden, ln_scale, w_q, w_k, w_v, w_gate, w_up, w_o, w_down, k_cache, v_cache, positions):
        q, kv_new, keep_e, recv_e, u, send, keep_0 = front(
            x_size, y_size, ge, sizes[0], hidden, ln_scale, w_q, w_k, w_v, w_gate, w_up
        )
        keep, recv = [keep_e, keep_0], [recv_e]
        at = ge + sizes[0]
        for c, n in enumerate(sizes):
            if c:
                send, k = gate_up(u, w_gate, w_up, at, n, 256)
                keep.append(k)
                at += n
            recv.append(lax.ppermute(send, "tpx", swap_x))

        cos_tab, sin_tab = rope_tables(positions, k_cache.shape[2])
        o, k_all, v_all = attention(q, kv_new, cos_tab, sin_tab, k_cache, v_cache, positions)
        hidden_out = tail(keep, recv, o, hidden, w_down, w_o)
        return hidden_out, k_all, v_all

    return jax.shard_map(device_step, mesh=mesh, in_specs=in_specs, out_specs=out_specs, check_vma=False)
```

```python
import functools

import jax
import jax.numpy as jnp
from jax import lax
from jax.experimental import pallas as pl
from jax.experimental.pallas import tpu as pltpu
from jax.sharding import PartitionSpec as P


LN_EPS = 1e-6
ROPE_BASE = 10000.0
MESH = pl.DeviceIdType.MESH
F32 = jnp.float32
BF16 = jnp.bfloat16


def rope_tables(positions, head_dim):
    half_dim = head_dim // 2
    inv_freq = ROPE_BASE ** (-(jnp.arange(half_dim, dtype=F32) * 2.0 / head_dim))
    angles = positions.astype(F32)[:, None] * inv_freq[None, :]
    return jnp.cos(angles), jnp.sin(angles)


def rope(x, cos, sin):
    half = x.shape[-1] // 2
    lead, tail = x[:, :half], x[:, half:]
    return jnp.concatenate([lead * cos - tail * sin, lead * sin + tail * cos], axis=-1)


def front_kernel(nx, ny, ge, gc, h_ref, sc_ref, wq_hbm, wk_hbm, wv_hbm, wg_hbm, wu_hbm,
                 q_hbm, kv_hbm, ke_hbm, re_hbm, u_hbm, gs_hbm, gk_hbm,
                 hbuf, scbuf, stat, cols, u_ref, wq, wkv, wgu, qs, qr, qo, kvs, kvr, es, er, ke, gs, gk, qn, qall, qf, kvn,
                 wsem, hs, hr, ss, sr, ts, tr, qss, qrs, ls, as_, ar, outs):
    ix, iy = lax.axis_index("tpx"), lax.axis_index("tpy")
    rows, width = h_ref.shape
    n_dev = nx * ny
    half = rows // 2
    n_seq = half // ny
    dim = wk_hbm.shape[1]
    gw = ge + gc
    partner = iy + 1 - 2 * lax.rem(iy, 2)
    cross = lax.rem(iy + 2, ny)
    diag = lax.rem(partner + 2, ny)
    me = ix * ny + iy
    peer_x = {"tpx": 1 - ix, "tpy": iy}

    def remote(src, dst, send, recv, dev):
        return pltpu.make_async_remote_copy(
            src_ref=src, dst_ref=dst, send_sem=send, recv_sem=recv, device_id=dev, device_id_type=MESH
        )

    loads = [
        pltpu.make_async_copy(wq_hbm, wq, wsem.at[0]),
        pltpu.make_async_copy(wk_hbm, wkv.at[0], wsem.at[1]),
        pltpu.make_async_copy(wv_hbm, wkv.at[1], wsem.at[2]),
        pltpu.make_async_copy(wg_hbm.at[:, 0:gw], wgu.at[0], wsem.at[3]),
        pltpu.make_async_copy(wu_hbm.at[:, 0:gw], wgu.at[1], wsem.at[4]),
    ]
    for c in loads:
        c.start()

    others = [(dx, dy) for dx in range(nx) for dy in range(ny) if dx or dy]
    barrier = pltpu.get_barrier_semaphore()
    for dx, dy in others:
        pl.semaphore_signal(
            barrier,
            inc=1,
            device_id={"tpx": lax.rem(ix + dx, nx), "tpy": lax.rem(iy + dy, ny)},
            device_id_type=MESH,
        )
    pl.semaphore_wait(barrier, n_dev - 1)

    chunks = [(0, 32), (32, half - 32), (half, half // 2), (half + half // 2, half // 2)]
    n_ch = len(chunks)

    def nat(j):
        r0, rn = chunks[j]
        base = (1 - ix) * half + r0 if r0 < half else ix * half + r0 - half
        return pl.ds(pl.multiple_of(base, 32), rn)

    def perm(j):
        return pl.ds(*chunks[j])

    def h_copy(j, dst_y, k):
        return remote(h_ref.at[nat(j)], hbuf.at[iy, perm(j)], hs.at[k, j], hr.at[k, j], {"tpx": ix, "tpy": dst_y})

    to_cross = [h_copy(j, cross, 0) for j in range(n_ch)]
    to_partner = [h_copy(j, partner, 1) for j in range(n_ch)]
    to_cross[0].start()
    for c in to_partner:
        c.start()

    hf = h_ref[...].astype(F32)
    total = jnp.sum(hf, axis=1, keepdims=True)
    dev = hf - total / width
    spread = jnp.sum(dev * dev, axis=1, keepdims=True)
    lane = lax.broadcasted_iota(jnp.int32, (rows, 128), 1)
    packed = jnp.where(lane == 0, total, jnp.where(lane == 1, spread, 0.0))
    stat[me] = jnp.transpose(packed)[:2]
    stat_copies = []
    for k, (dx, dy) in enumerate(others):
        c = remote(
            stat.at[me], stat.at[me], ts.at[k], tr.at[k],
            {"tpx": lax.rem(ix + dx, nx), "tpy": lax.rem(iy + dy, ny)},
        )
        c.start()
        stat_copies.append(c)
    sc_copies = []
    for k, dst in enumerate((cross, partner, diag)):
        c = remote(sc_ref, scbuf.at[iy], ss.at[k], sr.at[k], {"tpx": ix, "tpy": dst})
        c.start()
        sc_copies.append(c)
    for c in to_cross[1:]:
        c.start()

    forward = []

    def relay(j):
        to_cross[j].wait_recv()
        part = hbuf.at[cross, perm(j)]
        c = remote(part, part, hs.at[2, j], hr.at[2, j], {"tpx": ix, "tpy": partner})
        c.start()
        forward.append(c)

    relay(0)
    for c in stat_copies:
        c.wait_recv()
    sums = [stat[d, 0:1, :] for d in range(n_dev)]
    sprd = [stat[d, 1:2, :] for d in range(n_dev)]
    mean = functools.reduce(jnp.add, sums) / (width * n_dev)
    m2 = functools.reduce(jnp.add, sprd)
    for d in range(n_dev):
        gap = sums[d] / width - mean
        m2 = m2 + width * gap * gap
    rs = lax.rsqrt(m2 / (width * n_dev) + LN_EPS)
    sub = lax.broadcasted_iota(jnp.int32, (128, rows), 0)
    cols[...] = jnp.transpose(jnp.where(sub == 0, mean, jnp.where(sub == 1, rs, 0.0)))
    for c in sc_copies:
        c.wait_recv()

    def emit(block, scale, owner, j):
        stats = cols[nat(j), :]
        u = ((block.astype(F32) - stats[:, 0:1]) * stats[:, 1:2] * scale).astype(BF16)
        u_ref[perm(j), pl.ds(pl.multiple_of(owner * width, width), width)] = u

    def normalise(j):
        emit(h_ref[nat(j), :], sc_ref[...], iy, j)
        to_partner[j].wait_recv()
        emit(hbuf[partner, perm(j), :], scbuf[partner], partner, j)
        emit(hbuf[cross, perm(j), :], scbuf[cross], cross, j)
        forward[j].wait_recv()
        emit(hbuf[diag, perm(j), :], scbuf[diag], diag, j)

    def dot(a, b):
        return jnp.dot(a, b, preferred_element_type=F32)

    q_copies = []
    for j in range(n_ch):
        if 0 < j < n_ch - 1:
            relay(j + 1)
        normalise(j)
        if j < n_ch // 2:
            if j == 0:
                loads[0].wait()
            qs[perm(j), :] = dot(u_ref[perm(j), :], wq[...])
            c = remote(qs.at[perm(j)], qr.at[perm(j)], qss.at[j], qrs.at[j], peer_x)
            c.start()
            q_copies.append(c)
        if j == 0:
            relay(1)
    loads[1].wait()
    loads[2].wait()
    oth_rows = u_ref[pl.ds(pl.multiple_of(iy * n_seq, n_seq), n_seq), :]
    own_rows = u_ref[pl.ds(pl.multiple_of(half + iy * n_seq, n_seq), n_seq), :]
    for k in range(2):
        kvs[:, k * dim : (k + 1) * dim] = dot(oth_rows, wkv[k])
    kv_copy = remote(kvs, kvr, ls.at[0], ls.at[1], peer_x)
    kv_copy.start()
    u_out = pltpu.make_async_copy(u_ref, u_hbm, outs.at[0])
    u_out.start()
    loads[3].wait()
    loads[4].wait()
    for k in range(2):
        y = dot(u_ref[...], wgu[k, :, 0:ge])
        es[k] = y[:half]
        ke[k] = y[half:]
    e_copy = remote(es, er, ls.at[2], ls.at[3], peer_x)
    e_copy.start()
    ke_out = pltpu.make_async_copy(ke, ke_hbm, outs.at[3])
    ke_out.start()
    qo[...] = dot(u_ref[pl.ds(half, half), :], wq[...])
    own_kv = [dot(own_rows, wkv[k]) for k in range(2)]

    def gate_up_part(lo, hi):
        for k in range(2):
            y = dot(u_ref[...], wgu[k, :, ge + lo : ge + hi])
            gs[k, :, lo:hi] = y[:half]
            gk[k, :, lo:hi] = y[half:]

    gate_up_part(0, gc // 2)
    for j in range(n_ch // 2):
        q_copies[j].wait_recv()
        qn[perm(j), :] = (qo[perm(j), :] + qr[perm(j), :]).astype(BF16)
    q_sends = []
    for k in range(1, ny):
        d = lax.rem(iy + k, ny)
        c = remote(
            qn.at[pl.ds(pl.multiple_of(d * n_seq, n_seq), n_seq)], qall.at[iy],
            as_.at[k - 1], ar.at[k - 1], {"tpx": ix, "tpy": d},
        )
        c.start()
        q_sends.append(c)
    gate_up_part(gc // 2, gc)
    g_out = [pltpu.make_async_copy(gs, gs_hbm, outs.at[1]), pltpu.make_async_copy(gk, gk_hbm, outs.at[2])]
    for c in g_out:
        c.start()
    kv_copy.wait_recv()
    for k in range(2):
        sl = slice(k * dim, (k + 1) * dim)
        kvn[:, sl] = (own_kv[k] + kvr[:, sl]).astype(BF16)
    kv_out = pltpu.make_async_copy(kvn, kv_hbm, outs.at[4])
    kv_out.start()
    qf[iy] = qn[pl.ds(pl.multiple_of(iy * n_seq, n_seq), n_seq), :].astype(F32)
    for k in range(1, ny):
        q_sends[k - 1].wait_recv()
        src = lax.rem(iy + ny - k, ny)
        qf[src] = qall[src].astype(F32)
    q_out = pltpu.make_async_copy(qf, q_hbm, outs.at[5])
    q_out.start()
    e_copy.wait_recv()
    re_out = pltpu.make_async_copy(er, re_hbm, outs.at[6])
    re_out.start()
    for c in to_cross + to_partner + forward + sc_copies + stat_copies + q_copies + q_sends + [kv_copy, e_copy]:
        c.wait_send()
    for c in [u_out, ke_out, kv_out, q_out, re_out] + g_out:
        c.wait()


def front(nx, ny, ge, gc, hidden, ln_scale, w_q, w_k, w_v, w_gate, w_up):
    rows, width = hidden.shape
    half = rows // 2
    n_dev, n_seq = nx * ny, rows // (nx * ny)
    kdim, nq = w_q.shape
    dim = w_k.shape[1]
    vm = pl.BlockSpec(memory_space=pltpu.VMEM)
    hbm = pl.BlockSpec(memory_space=pltpu.HBM)
    dma = pltpu.SemaphoreType.DMA
    sds = jax.ShapeDtypeStruct
    return pl.pallas_call(
        functools.partial(front_kernel, nx, ny, ge, gc),
        out_shape=[
            sds((ny, n_seq, nq), F32),
            sds((n_seq, 2 * dim), BF16),
            sds((2, half, ge), F32),
            sds((2, half, ge), F32),
            sds((rows, kdim), BF16),
            sds((2, half, gc), F32),
            sds((2, half, gc), F32),
        ],
        in_specs=[vm, vm] + [hbm] * 5,
        out_specs=[hbm] * 7,
        scratch_shapes=[
            pltpu.VMEM((ny, rows, width), BF16),
            pltpu.VMEM((ny, 1, width), F32),
            pltpu.VMEM((n_dev, 2, rows), F32),
            pltpu.VMEM((rows, 128), F32),
            pltpu.VMEM((rows, kdim), BF16),
            pltpu.VMEM((kdim, nq), BF16),
            pltpu.VMEM((2, kdim, dim), BF16),
            pltpu.VMEM((2, kdim, ge + gc), BF16),
            pltpu.VMEM((half, nq), F32),
            pltpu.VMEM((half, nq), F32),
            pltpu.VMEM((half, nq), F32),
            pltpu.VMEM((n_seq, 2 * dim), F32),
            pltpu.VMEM((n_seq, 2 * dim), F32),
            pltpu.VMEM((2, half, ge), F32),
            pltpu.VMEM((2, half, ge), F32),
            pltpu.VMEM((2, half, ge), F32),
            pltpu.VMEM((2, half, gc), F32),
            pltpu.VMEM((2, half, gc), F32),
            pltpu.VMEM((half, nq), BF16),
            pltpu.VMEM((ny, n_seq, nq), BF16),
            pltpu.VMEM((ny, n_seq, nq), F32),
            pltpu.VMEM((n_seq, 2 * dim), BF16),
            dma((5,)),
            dma((3, 4)),
            dma((3, 4)),
            dma((3,)),
            dma((3,)),
            dma((n_dev - 1,)),
            dma((n_dev - 1,)),
            dma((2,)),
            dma((2,)),
            dma((4,)),
            dma((ny - 1,)),
            dma((ny - 1,)),
            dma((7,)),
        ],
        compiler_params=pltpu.CompilerParams(collective_id=0, has_side_effects=True, vmem_limit_bytes=56 * 2**20),
        cost_estimate=pl.CostEstimate(flops=2 * rows * kdim * nq, bytes_accessed=2 * kdim * nq, transcendentals=0),
        name="front",
    )(hidden, ln_scale.reshape(1, width), w_q, w_k, w_v, w_gate, w_up)


def gu_kernel(u_ref, wg_ref, wu_ref, send, keep):
    half = u_ref.shape[0] // 2
    for k, w_ref in enumerate((wg_ref, wu_ref)):
        y = jnp.dot(u_ref[...], w_ref[...], preferred_element_type=F32)
        send[k] = y[:half]
        keep[k] = y[half:]


def gate_up(u, w_gate, w_up, start, cols, blk):
    rows, kdim = u.shape
    half = rows // 2
    first = start // blk
    shape = jax.ShapeDtypeStruct((2, half, cols), F32)
    wspec = pl.BlockSpec((kdim, blk), lambda i: (0, i + first))
    ospec = pl.BlockSpec((2, half, blk), lambda i: (0, 0, i))
    return pl.pallas_call(
        gu_kernel,
        grid=(cols // blk,),
        out_shape=[shape, shape],
        in_specs=[pl.BlockSpec((rows, kdim), lambda i: (0, 0)), wspec, wspec],
        out_specs=[ospec, ospec],
        compiler_params=pltpu.CompilerParams(vmem_limit_bytes=56 * 2**20),
        cost_estimate=pl.CostEstimate(
            flops=4 * rows * kdim * cols, bytes_accessed=4 * kdim * cols, transcendentals=0
        ),
        name="gate_up",
    )(u, w_gate, w_up)


def attn_kernel(nb, ahead, pos_ref, q_ref, kv_ref, cos_ref, sin_ref, kc_ref, vc_ref,
                o_ref, ko_ref, vo_ref, kbuf, vbuf, krow, vrow, qrot, orow, ki, vi, ks, vs):
    n_seq, n_head, dim = qrot.shape
    n_dev = q_ref.shape[0]
    per = n_head // n_dev
    length = kbuf.shape[1]

    def fetch(b, slot):
        pltpu.make_async_copy(kc_ref.at[b], kbuf.at[slot], ki.at[slot]).start()
        pltpu.make_async_copy(vc_ref.at[b], vbuf.at[slot], vi.at[slot]).start()

    def wait_out(b, slot):
        pltpu.make_async_copy(kbuf.at[slot], ko_ref.at[b], ks.at[slot]).wait()
        pltpu.make_async_copy(vbuf.at[slot], vo_ref.at[b], vs.at[slot]).wait()

    for b in range(ahead):
        fetch(b, b)
    krow[...] = rope(kv_ref[:, :dim].astype(F32), cos_ref[...], sin_ref[...]).astype(BF16).astype(F32)
    vrow[...] = kv_ref[:, dim:].astype(F32)
    for d in range(n_dev):
        for h in range(per):
            x = rope(q_ref[d, :, h * dim : (h + 1) * dim], cos_ref[...], sin_ref[...])
            qrot[:, d * per + h, :] = x

    def patch(buf, slot, row, p):
        base = pl.multiple_of((p // 16) * 16, 16)
        old = buf[slot, pl.ds(base, 16), :].astype(F32)
        hit = lax.broadcasted_iota(jnp.int32, old.shape, 0) == p - base
        buf[slot, pl.ds(base, 16), :] = jnp.where(hit, row, old).astype(BF16)

    @pl.loop(0, n_seq // 2)
    def _(i):
        work = []
        for j in range(2):
            b = 2 * i + j
            slot = lax.rem(b, nb)
            nxt = b + ahead
            nslot = lax.rem(nxt, nb)

            @pl.when(jnp.logical_and(nxt < n_seq, nxt >= nb))
            def _():
                wait_out(nxt - nb, nslot)

            @pl.when(nxt < n_seq)
            def _():
                fetch(nxt, nslot)

            work.append((b, slot))
        for b, slot in work:
            p = pos_ref[b]
            pltpu.make_async_copy(kc_ref.at[b], kbuf.at[slot], ki.at[slot]).wait()
            patch(kbuf, slot, krow[pl.ds(b, 1), :], p)
            pltpu.make_async_copy(vc_ref.at[b], vbuf.at[slot], vi.at[slot]).wait()
            patch(vbuf, slot, vrow[pl.ds(b, 1), :], p)
        for b, slot in work:
            p = pos_ref[b]
            q = qrot[b].astype(BF16)
            s = lax.dot_general(q, kbuf[slot], (((1,), (1,)), ((), ())), preferred_element_type=F32)
            s = s * (dim ** -0.5)
            ok = lax.broadcasted_iota(jnp.int32, (n_head, length), 1) <= p
            s = jnp.where(ok, s, -jnp.inf)
            e = jnp.exp(s - jnp.max(s, axis=1, keepdims=True))
            prob = (e / jnp.sum(e, axis=1, keepdims=True)).astype(BF16)
            o = jnp.dot(prob, vbuf[slot], preferred_element_type=F32)
            for h in range(n_head):
                orow[h // per, pl.ds(b, 1), (h % per) * dim : (h % per + 1) * dim] = o[h : h + 1]
        for b, slot in work:
            pltpu.make_async_copy(kbuf.at[slot], ko_ref.at[b], ks.at[slot]).start()
            pltpu.make_async_copy(vbuf.at[slot], vo_ref.at[b], vs.at[slot]).start()

    o_ref[...] = orow[...].astype(BF16)
    for b in range(n_seq - nb, n_seq):
        wait_out(b, b % nb)


def attention(q, kv_new, cos, sin, k_cache, v_cache, positions, nb=8, ahead=4):
    n_seq, length, dim = k_cache.shape
    n_head = q.shape[0] * q.shape[2] // dim
    vm = pl.BlockSpec(memory_space=pltpu.VMEM)
    hbm = pl.BlockSpec(memory_space=pltpu.HBM)
    return pl.pallas_call(
        functools.partial(attn_kernel, nb, ahead),
        out_shape=[
            jax.ShapeDtypeStruct(q.shape, BF16),
            jax.ShapeDtypeStruct(k_cache.shape, BF16),
            jax.ShapeDtypeStruct(v_cache.shape, BF16),
        ],
        in_specs=[pl.BlockSpec(memory_space=pltpu.SMEM), vm, vm, vm, vm, hbm, hbm],
        out_specs=[vm, hbm, hbm],
        scratch_shapes=[
            pltpu.VMEM((nb, length, dim), BF16),
            pltpu.VMEM((nb, length, dim), BF16),
            pltpu.VMEM((n_seq, dim), F32),
            pltpu.VMEM((n_seq, dim), F32),
            pltpu.VMEM((n_seq, n_head, dim), F32),
            pltpu.VMEM(q.shape, F32),
            pltpu.SemaphoreType.DMA((nb,)),
            pltpu.SemaphoreType.DMA((nb,)),
            pltpu.SemaphoreType.DMA((nb,)),
            pltpu.SemaphoreType.DMA((nb,)),
        ],
        compiler_params=pltpu.CompilerParams(vmem_limit_bytes=40 * 2**20),
        cost_estimate=pl.CostEstimate(
            flops=4 * 10**10, bytes_accessed=8 * n_seq * length * dim, transcendentals=n_seq * n_head * length
        ),
        name="attention",
    )(positions, q, kv_new, cos, sin, k_cache, v_cache)


def tail_kernel(n_gu, cuts, n_w, *refs):
    keeps, recvs = refs[:n_gu], refs[n_gu : 2 * n_gu]
    (o_ref, wd_hbm, wo_hbm, out_ref, wd, kbuf, rbuf, aown, aoth, give, hold, got1, pass_, got2,
     wsem, ksem, rsem, as_, ar, s1, r1, s2, r2, os_, or_) = refs[2 * n_gu :]
    ix, iy = lax.axis_index("tpx"), lax.axis_index("tpy")
    half = aown.shape[0]
    ny, n_seq = o_ref.shape[0], o_ref.shape[1]
    starts, at = [], 0
    for ref in keeps:
        starts.append((at, ref.shape[2]))
        at += ref.shape[2]
    width = out_ref.shape[1]
    kact, ko = wd_hbm.shape[0], wo_hbm.shape[0]
    partner = iy + 1 - 2 * lax.rem(iy, 2)
    cross = lax.rem(iy + 2, 4)
    core, chip = lax.rem(iy, 2), iy // 2
    peer_x = {"tpx": 1 - ix, "tpy": iy}
    peer_core = {"tpx": ix, "tpy": partner}
    peer_chip = {"tpx": ix, "tpy": cross}

    gu_loads = []
    for r, (r0, rn) in enumerate(cuts):
        group = []
        rows = pl.ds(r0, rn)
        for g in range(n_gu):
            part = pl.ds(*starts[g])
            group.append(pltpu.make_async_copy(keeps[g].at[:, rows], kbuf.at[:, rows, part], ksem.at[r, g]))
            group.append(pltpu.make_async_copy(recvs[g].at[:, rows], rbuf.at[:, rows, part], rsem.at[r, g]))
        for c in group:
            c.start()
        gu_loads.append(group)
    step = kact // n_w
    w_loads = []
    for j in range(n_w + 1):
        if j < n_w:
            src, dst = wd_hbm.at[pl.ds(j * step, step)], wd.at[pl.ds(j * step, step)]
        else:
            src, dst = wo_hbm, wd.at[pl.ds(kact, ko)]
        c = pltpu.make_async_copy(src, dst, wsem.at[j])
        c.start()
        w_loads.append(c)

    barrier = pltpu.get_barrier_semaphore()
    others = [(dx, dy) for dx in (1, 0) for dy in range(ny) if dx or dy]

    def shifted(dx, dy):
        return {"tpx": lax.rem(ix + dx, 2), "tpy": lax.rem(iy + dy, ny)}

    for dx, dy in others:
        pl.semaphore_signal(barrier, inc=1, device_id=shifted(dx, dy), device_id_type=MESH)
    pl.semaphore_wait(barrier, len(others))

    o_rows = pl.ds(pl.multiple_of(iy * n_seq, n_seq), n_seq)
    o_cols = pl.ds(kact, ko)
    o_copies = []
    for k, (dx, dy) in enumerate(others):
        c = pltpu.make_async_remote_copy(
            src_ref=o_ref.at[lax.rem(iy + dy, ny)],
            dst_ref=(aoth if dx else aown).at[o_rows, o_cols],
            send_sem=os_.at[k],
            recv_sem=or_.at[k],
            device_id=shifted(dx, dy),
            device_id_type=MESH,
        )
        c.start()
        o_copies.append(c)
    aown[o_rows, kact:] = o_ref[iy]

    sends = []
    for r, (r0, rn) in enumerate(cuts):
        rows = pl.ds(r0, rn)
        for c in gu_loads[r]:
            c.wait()
        for g in range(n_gu):
            part = pl.ds(*starts[g])
            gate = (kbuf[0, rows, part] + rbuf[0, rows, part]).astype(BF16).astype(F32)
            up = (kbuf[1, rows, part] + rbuf[1, rows, part]).astype(BF16).astype(F32)
            aown[rows, part] = (jax.nn.silu(gate) * up).astype(BF16)
        c = pltpu.make_async_remote_copy(
            src_ref=aown.at[rows, pl.ds(0, kact)],
            dst_ref=aoth.at[rows, pl.ds(0, kact)],
            send_sem=as_.at[r],
            recv_sem=ar.at[r],
            device_id=peer_x,
            device_id_type=MESH,
        )
        c.start()
        sends.append(c)
    for c in w_loads:
        c.wait()
    for c in o_copies:
        c.wait_recv()

    blocks = [(half, half)] + [(r0, rn) for r0, rn in cuts]

    def product(lhs, x, c):
        col = pl.ds(pl.multiple_of((x * 2 + c) * width, width), width)
        return jnp.dot(lhs, wd[:, col], preferred_element_type=F32)

    stage1, stage2 = [], []

    def give_block(k, rows, lhs, x):
        give[x, rows, :] = product(lhs, x, 1 - core)
        c = pltpu.make_async_remote_copy(
            src_ref=give.at[x, rows],
            dst_ref=got1.at[x, rows],
            send_sem=s1.at[k, len(stage1[k])],
            recv_sem=r1.at[k, len(stage1[k])],
            device_id=peer_core,
            device_id_type=MESH,
        )
        c.start()
        stage1[k].append(c)

    def reduce_block(k):
        r0, rn = blocks[k]
        rows = pl.ds(r0, rn)
        stage1[k][0].wait_recv()
        pass_[rows, :] = hold[0, rows, :] + got1[1 - chip, rows, :]
        c = pltpu.make_async_remote_copy(
            src_ref=pass_.at[rows],
            dst_ref=got2.at[rows],
            send_sem=s2.at[k],
            recv_sem=r2.at[k],
            device_id=peer_chip,
            device_id_type=MESH,
        )
        c.start()
        stage2.append(c)

    def run_block(k, last):
        r0, rn = blocks[k]
        rows = pl.ds(r0, rn)
        stage1.append([])
        if k == 0:
            lhs = aown[...]
        else:
            sends[k - 1].wait_recv()
            lhs = aoth[rows, :]
        give_block(k, rows, lhs, 1 - chip)
        hold[0, rows, :] = product(lhs, 1 - chip, core)
        if k:
            reduce_block(k - 1)
        give_block(k, rows, lhs, chip)
        if last:
            reduce_block(k)
        hold[1, rows, :] = product(lhs, chip, core)

    def finish_block(k):
        r0, rn = blocks[k]
        rows = pl.ds(r0, rn)
        stage1[k][1].wait_recv()
        partial = hold[1, rows, :] + got1[chip, rows, :]
        stage2[k].wait_recv()
        base = ix * half if k == 0 else (1 - ix) * half + r0
        out_ref[pl.ds(pl.multiple_of(base, 16), rn), :] = partial + got2[rows, :]

    n_blk = len(blocks)
    for k in range(n_blk):
        run_block(k, k == n_blk - 1)
    for k in range(n_blk):
        finish_block(k)
    for c in sends + [c for g in stage1 for c in g] + stage2 + o_copies:
        c.wait_send()


def tail(keeps, recvs, o, rows, width, w_down, w_o):
    n_gu = len(keeps)
    half = keeps[0].shape[1]
    n = w_down.shape[1]
    kdim = w_down.shape[0] + w_o.shape[0]
    cuts = [(0, 64), (64, 32), (96, 16), (112, 16)]
    n_w, n_cut, n_blk = 8, len(cuts), len(cuts) + 1
    vm = pl.BlockSpec(memory_space=pltpu.VMEM)
    hbm = pl.BlockSpec(memory_space=pltpu.HBM)
    dma = pltpu.SemaphoreType.DMA
    return pl.pallas_call(
        functools.partial(tail_kernel, n_gu, cuts, n_w),
        out_shape=jax.ShapeDtypeStruct((rows, width), F32),
        in_specs=[hbm] * (2 * n_gu) + [vm] + [hbm] * 2,
        out_specs=vm,
        scratch_shapes=[
            pltpu.VMEM((kdim, n), BF16),
            pltpu.VMEM((2, half, w_down.shape[0]), F32),
            pltpu.VMEM((2, half, w_down.shape[0]), F32),
            pltpu.VMEM((half, kdim), BF16),
            pltpu.VMEM((half, kdim), BF16),
            pltpu.VMEM((2, rows, width), F32),
            pltpu.VMEM((2, rows, width), F32),
            pltpu.VMEM((2, rows, width), F32),
            pltpu.VMEM((rows, width), F32),
            pltpu.VMEM((rows, width), F32),
            dma((n_w + 1,)),
            dma((n_cut, n_gu)),
            dma((n_cut, n_gu)),
            dma((n_cut,)),
            dma((n_cut,)),
            dma((n_blk, 2)),
            dma((n_blk, 2)),
            dma((n_blk,)),
            dma((n_blk,)),
            dma((7,)),
            dma((7,)),
        ],
        compiler_params=pltpu.CompilerParams(collective_id=1, has_side_effects=True, vmem_limit_bytes=44 * 2**20),
        cost_estimate=pl.CostEstimate(flops=2 * rows * kdim * n, bytes_accessed=2 * kdim * n, transcendentals=0),
        name="tail",
    )(*keeps, *recvs, o, w_down, w_o)


def solution(mesh):
    x_size = mesh.shape["tpx"]
    y_size = mesh.shape["tpy"]
    hidden_spec = P("dp", ("tpx", "tpy"))
    cache_spec = P(("dp", "tpx", "tpy"), None, None)
    in_specs = (hidden_spec, P(("tpx", "tpy")), P("tpx", "tpy"), P("tpx", None), P("tpx", None), P("tpx", "tpy"), P("tpx", "tpy"), P("tpy", "tpx"), P("tpy", "tpx"), cache_spec, cache_spec, P(("dp", "tpx", "tpy")))
    out_specs = (hidden_spec, cache_spec, cache_spec)
    swap_x = [(0, 1), (1, 0)]
    ge, sizes = 256, (1024, 1024, 1024, 768)

    def device_step(hidden, ln_scale, w_q, w_k, w_v, w_gate, w_up, w_o, w_down, k_cache, v_cache, positions):
        q, kv_new, keep_e, recv_e, u, send, keep_0 = front(
            x_size, y_size, ge, sizes[0], hidden, ln_scale, w_q, w_k, w_v, w_gate, w_up
        )
        keep, recv = [keep_e, keep_0], [recv_e]
        at = ge + sizes[0]
        for c, n in enumerate(sizes):
            if c:
                send, k = gate_up(u, w_gate, w_up, at, n, 256)
                keep.append(k)
                at += n
            recv.append(lax.ppermute(send, "tpx", swap_x))

        cos_tab, sin_tab = rope_tables(positions, k_cache.shape[2])
        o, k_all, v_all = attention(q, kv_new, cos_tab, sin_tab, k_cache, v_cache, positions)
        total = tail(keep, recv, o, *hidden.shape, w_down, w_o)
        hidden_out = (hidden.astype(F32) + total).astype(BF16)
        return hidden_out, k_all, v_all

    return jax.shard_map(device_step, mesh=mesh, in_specs=in_specs, out_specs=out_specs, check_vma=False)
```

```python
import functools

import jax
import jax.numpy as jnp
from jax import lax
from jax.experimental import pallas as pl
from jax.experimental.pallas import tpu as pltpu
from jax.sharding import PartitionSpec as P


LN_EPS = 1e-6
ROPE_BASE = 10000.0
MESH = pl.DeviceIdType.MESH
F32 = jnp.float32
BF16 = jnp.bfloat16


def rope_tables(positions, head_dim):
    half_dim = head_dim // 2
    inv_freq = ROPE_BASE ** (-(jnp.arange(half_dim, dtype=F32) * 2.0 / head_dim))
    angles = positions.astype(F32)[:, None] * inv_freq[None, :]
    return jnp.cos(angles), jnp.sin(angles)


def rope(x, cos, sin):
    half = x.shape[-1] // 2
    lead, tail = x[:, :half], x[:, half:]
    return jnp.concatenate([lead * cos - tail * sin, lead * sin + tail * cos], axis=-1)


def front_kernel(nx, ny, ge, gc, h_ref, sc_ref, wq_hbm, wk_hbm, wv_hbm, wg_hbm, wu_hbm,
                 q_hbm, kv_hbm, ke_hbm, re_hbm, u_hbm, gs_hbm, gk_hbm,
                 hbuf, scbuf, stat, cols, u_ref, wq, wkv, wgu, qs, qr, qo, kvs, kvr, es, ke, gs, gk, qn, qall, qf, kvn,
                 wsem, hs, hr, ss, sr, ts, tr, qss, qrs, ls, as_, ar, outs):
    ix, iy = lax.axis_index("tpx"), lax.axis_index("tpy")
    rows, width = h_ref.shape
    n_dev = nx * ny
    half = rows // 2
    n_seq = half // ny
    dim = wk_hbm.shape[1]
    gw = ge + gc
    partner = iy + 1 - 2 * lax.rem(iy, 2)
    cross = lax.rem(iy + 2, ny)
    diag = lax.rem(partner + 2, ny)
    me = ix * ny + iy
    peer_x = {"tpx": 1 - ix, "tpy": iy}

    def remote(src, dst, send, recv, dev):
        return pltpu.make_async_remote_copy(
            src_ref=src, dst_ref=dst, send_sem=send, recv_sem=recv, device_id=dev, device_id_type=MESH
        )

    loads = [
        pltpu.make_async_copy(wq_hbm, wq, wsem.at[0]),
        pltpu.make_async_copy(wk_hbm, wkv.at[0], wsem.at[1]),
        pltpu.make_async_copy(wv_hbm, wkv.at[1], wsem.at[2]),
        pltpu.make_async_copy(wg_hbm.at[:, 0:gw], wgu.at[0], wsem.at[3]),
        pltpu.make_async_copy(wu_hbm.at[:, 0:gw], wgu.at[1], wsem.at[4]),
    ]
    for c in loads:
        c.start()

    others = [(dx, dy) for dx in range(nx) for dy in range(ny) if dx or dy]
    barrier = pltpu.get_barrier_semaphore()
    for dx, dy in others:
        pl.semaphore_signal(
            barrier,
            inc=1,
            device_id={"tpx": lax.rem(ix + dx, nx), "tpy": lax.rem(iy + dy, ny)},
            device_id_type=MESH,
        )
    hf = h_ref[...].astype(F32)
    total = jnp.sum(hf, axis=1, keepdims=True)
    dev = hf - total / width
    spread = jnp.sum(dev * dev, axis=1, keepdims=True)
    lane = lax.broadcasted_iota(jnp.int32, (rows, 128), 1)
    packed = jnp.where(lane == 0, total, jnp.where(lane == 1, spread, 0.0))
    stat[me] = jnp.transpose(packed)[:2]
    pl.semaphore_wait(barrier, n_dev - 1)

    chunks = [(0, 32), (32, half - 32), (half, half // 2), (half + half // 2, half // 2)]
    n_ch = len(chunks)

    def nat(j):
        r0, rn = chunks[j]
        base = (1 - ix) * half + r0 if r0 < half else ix * half + r0 - half
        return pl.ds(pl.multiple_of(base, 32), rn)

    def perm(j):
        return pl.ds(*chunks[j])

    def h_copy(j, dst_y, k):
        return remote(h_ref.at[nat(j)], hbuf.at[iy, perm(j)], hs.at[k, j], hr.at[k, j], {"tpx": ix, "tpy": dst_y})

    to_cross = [h_copy(j, cross, 0) for j in range(n_ch)]
    to_partner = [h_copy(j, partner, 1) for j in range(n_ch)]
    to_cross[0].start()
    stat_copies = []
    for k, (dx, dy) in enumerate(others):
        c = remote(
            stat.at[me], stat.at[me], ts.at[k], tr.at[k],
            {"tpx": lax.rem(ix + dx, nx), "tpy": lax.rem(iy + dy, ny)},
        )
        c.start()
        stat_copies.append(c)
    for c in to_partner:
        c.start()

    sc_copies = []
    for k, dst in enumerate((cross, partner, diag)):
        c = remote(sc_ref, scbuf.at[iy], ss.at[k], sr.at[k], {"tpx": ix, "tpy": dst})
        c.start()
        sc_copies.append(c)
    for c in to_cross[1:]:
        c.start()

    forward = []

    def relay(j):
        to_cross[j].wait_recv()
        part = hbuf.at[cross, perm(j)]
        c = remote(part, part, hs.at[2, j], hr.at[2, j], {"tpx": ix, "tpy": partner})
        c.start()
        forward.append(c)

    relay(0)
    for c in stat_copies:
        c.wait_recv()
    sums = [stat[d, 0:1, :] for d in range(n_dev)]
    sprd = [stat[d, 1:2, :] for d in range(n_dev)]
    mean = functools.reduce(jnp.add, sums) / (width * n_dev)
    m2 = functools.reduce(jnp.add, sprd)
    for d in range(n_dev):
        gap = sums[d] / width - mean
        m2 = m2 + width * gap * gap
    rs = lax.rsqrt(m2 / (width * n_dev) + LN_EPS)
    sub = lax.broadcasted_iota(jnp.int32, (128, rows), 0)
    cols[...] = jnp.transpose(jnp.where(sub == 0, mean, jnp.where(sub == 1, rs, 0.0)))
    for c in sc_copies:
        c.wait_recv()

    def emit(block, scale, owner, j):
        stats = cols[nat(j), :]
        u = ((block.astype(F32) - stats[:, 0:1]) * stats[:, 1:2] * scale).astype(BF16)
        u_ref[perm(j), pl.ds(pl.multiple_of(owner * width, width), width)] = u

    def normalise(j):
        emit(h_ref[nat(j), :], sc_ref[...], iy, j)
        to_partner[j].wait_recv()
        emit(hbuf[partner, perm(j), :], scbuf[partner], partner, j)
        emit(hbuf[cross, perm(j), :], scbuf[cross], cross, j)
        forward[j].wait_recv()
        emit(hbuf[diag, perm(j), :], scbuf[diag], diag, j)

    def dot(a, b):
        return jnp.dot(a, b, preferred_element_type=F32)

    q_copies = []
    for j in range(n_ch):
        if 0 < j < n_ch - 1:
            relay(j + 1)
        normalise(j)
        if j < n_ch // 2:
            if j == 0:
                loads[0].wait()
            qs[perm(j), :] = dot(u_ref[perm(j), :], wq[...])
            c = remote(qs.at[perm(j)], qr.at[perm(j)], qss.at[j], qrs.at[j], peer_x)
            c.start()
            q_copies.append(c)
        if j == 0:
            relay(1)
    loads[1].wait()
    loads[2].wait()
    oth_rows = u_ref[pl.ds(pl.multiple_of(iy * n_seq, n_seq), n_seq), :]
    own_rows = u_ref[pl.ds(pl.multiple_of(half + iy * n_seq, n_seq), n_seq), :]
    for k in range(2):
        kvs[:, k * dim : (k + 1) * dim] = dot(oth_rows, wkv[k])
    kv_copy = remote(kvs, kvr, ls.at[0], ls.at[1], peer_x)
    kv_copy.start()
    u_out = pltpu.make_async_copy(u_ref, u_hbm, outs.at[0])
    u_out.start()
    loads[3].wait()
    loads[4].wait()
    for k in range(2):
        y = dot(u_ref[...], wgu[k, :, 0:ge])
        es[k] = y[:half]
        ke[k] = y[half:]
    e_copy = remote(es, re_hbm, ls.at[2], ls.at[3], peer_x)
    e_copy.start()
    ke_out = pltpu.make_async_copy(ke, ke_hbm, outs.at[3])
    ke_out.start()
    qo[...] = dot(u_ref[pl.ds(half, half), :], wq[...])
    own_kv = [dot(own_rows, wkv[k]) for k in range(2)]

    def gate_up_part(lo, hi):
        for k in range(2):
            y = dot(u_ref[...], wgu[k, :, ge + lo : ge + hi])
            gs[k, :, lo:hi] = y[:half]
            gk[k, :, lo:hi] = y[half:]

    gate_up_part(0, gc // 2)
    for j in range(n_ch // 2):
        q_copies[j].wait_recv()
        qn[perm(j), :] = (qo[perm(j), :] + qr[perm(j), :]).astype(BF16)
    q_sends = []
    for k in range(1, ny):
        d = lax.rem(iy + k, ny)
        c = remote(
            qn.at[pl.ds(pl.multiple_of(d * n_seq, n_seq), n_seq)], qall.at[iy],
            as_.at[k - 1], ar.at[k - 1], {"tpx": ix, "tpy": d},
        )
        c.start()
        q_sends.append(c)
    gate_up_part(gc // 2, gc)
    g_out = [pltpu.make_async_copy(gs, gs_hbm, outs.at[1]), pltpu.make_async_copy(gk, gk_hbm, outs.at[2])]
    for c in g_out:
        c.start()
    kv_copy.wait_recv()
    for k in range(2):
        sl = slice(k * dim, (k + 1) * dim)
        kvn[:, sl] = (own_kv[k] + kvr[:, sl]).astype(BF16)
    kv_out = pltpu.make_async_copy(kvn, kv_hbm, outs.at[4])
    kv_out.start()
    qf[iy] = qn[pl.ds(pl.multiple_of(iy * n_seq, n_seq), n_seq), :].astype(F32)
    for k in range(1, ny):
        q_sends[k - 1].wait_recv()
        src = lax.rem(iy + ny - k, ny)
        qf[src] = qall[src].astype(F32)
    q_out = pltpu.make_async_copy(qf, q_hbm, outs.at[5])
    q_out.start()
    e_copy.wait_recv()
    for c in to_cross + to_partner + forward + sc_copies + stat_copies + q_copies + q_sends + [kv_copy, e_copy]:
        c.wait_send()
    for c in [u_out, ke_out, kv_out, q_out] + g_out:
        c.wait()


def front(nx, ny, ge, gc, hidden, ln_scale, w_q, w_k, w_v, w_gate, w_up):
    rows, width = hidden.shape
    half = rows // 2
    n_dev, n_seq = nx * ny, rows // (nx * ny)
    kdim, nq = w_q.shape
    dim = w_k.shape[1]
    vm = pl.BlockSpec(memory_space=pltpu.VMEM)
    hbm = pl.BlockSpec(memory_space=pltpu.HBM)
    dma = pltpu.SemaphoreType.DMA
    sds = jax.ShapeDtypeStruct
    return pl.pallas_call(
        functools.partial(front_kernel, nx, ny, ge, gc),
        out_shape=[
            sds((ny, n_seq, nq), F32),
            sds((n_seq, 2 * dim), BF16),
            sds((2, half, ge), F32),
            sds((2, half, ge), F32),
            sds((rows, kdim), BF16),
            sds((2, half, gc), F32),
            sds((2, half, gc), F32),
        ],
        in_specs=[vm, vm] + [hbm] * 5,
        out_specs=[hbm] * 7,
        scratch_shapes=[
            pltpu.VMEM((ny, rows, width), BF16),
            pltpu.VMEM((ny, 1, width), F32),
            pltpu.VMEM((n_dev, 2, rows), F32),
            pltpu.VMEM((rows, 128), F32),
            pltpu.VMEM((rows, kdim), BF16),
            pltpu.VMEM((kdim, nq), BF16),
            pltpu.VMEM((2, kdim, dim), BF16),
            pltpu.VMEM((2, kdim, ge + gc), BF16),
            pltpu.VMEM((half, nq), F32),
            pltpu.VMEM((half, nq), F32),
            pltpu.VMEM((half, nq), F32),
            pltpu.VMEM((n_seq, 2 * dim), F32),
            pltpu.VMEM((n_seq, 2 * dim), F32),
            pltpu.VMEM((2, half, ge), F32),
            pltpu.VMEM((2, half, ge), F32),
            pltpu.VMEM((2, half, gc), F32),
            pltpu.VMEM((2, half, gc), F32),
            pltpu.VMEM((half, nq), BF16),
            pltpu.VMEM((ny, n_seq, nq), BF16),
            pltpu.VMEM((ny, n_seq, nq), F32),
            pltpu.VMEM((n_seq, 2 * dim), BF16),
            dma((5,)),
            dma((3, 4)),
            dma((3, 4)),
            dma((3,)),
            dma((3,)),
            dma((n_dev - 1,)),
            dma((n_dev - 1,)),
            dma((2,)),
            dma((2,)),
            dma((4,)),
            dma((ny - 1,)),
            dma((ny - 1,)),
            dma((6,)),
        ],
        compiler_params=pltpu.CompilerParams(collective_id=0, has_side_effects=True, vmem_limit_bytes=56 * 2**20),
        cost_estimate=pl.CostEstimate(flops=2 * rows * kdim * nq, bytes_accessed=2 * kdim * nq, transcendentals=0),
        name="front",
    )(hidden, ln_scale.reshape(1, width), w_q, w_k, w_v, w_gate, w_up)


def gu_kernel(u_ref, wg_ref, wu_ref, send, keep):
    half = u_ref.shape[0] // 2
    for k, w_ref in enumerate((wg_ref, wu_ref)):
        y = jnp.dot(u_ref[...], w_ref[...], preferred_element_type=F32)
        send[k] = y[:half]
        keep[k] = y[half:]


def gate_up(u, w_gate, w_up, start, cols, blk):
    rows, kdim = u.shape
    half = rows // 2
    first = start // blk
    shape = jax.ShapeDtypeStruct((2, half, cols), F32)
    wspec = pl.BlockSpec((kdim, blk), lambda i: (0, i + first))
    ospec = pl.BlockSpec((2, half, blk), lambda i: (0, 0, i))
    return pl.pallas_call(
        gu_kernel,
        grid=(cols // blk,),
        out_shape=[shape, shape],
        in_specs=[pl.BlockSpec((rows, kdim), lambda i: (0, 0)), wspec, wspec],
        out_specs=[ospec, ospec],
        compiler_params=pltpu.CompilerParams(vmem_limit_bytes=56 * 2**20),
        cost_estimate=pl.CostEstimate(
            flops=4 * rows * kdim * cols, bytes_accessed=4 * kdim * cols, transcendentals=0
        ),
        name="gate_up",
    )(u, w_gate, w_up)


def attn_kernel(nb, ahead, pos_ref, q_ref, kv_ref, cos_ref, sin_ref, kc_ref, vc_ref,
                o_ref, ko_ref, vo_ref, kbuf, vbuf, krow, vrow, qrot, orow, ki, vi, ks, vs):
    n_seq, n_head, dim = qrot.shape
    n_dev = q_ref.shape[0]
    per = n_head // n_dev
    length = kbuf.shape[1]

    def fetch(b, slot):
        pltpu.make_async_copy(kc_ref.at[b], kbuf.at[slot], ki.at[slot]).start()
        pltpu.make_async_copy(vc_ref.at[b], vbuf.at[slot], vi.at[slot]).start()

    def wait_out(b, slot):
        pltpu.make_async_copy(kbuf.at[slot], ko_ref.at[b], ks.at[slot]).wait()
        pltpu.make_async_copy(vbuf.at[slot], vo_ref.at[b], vs.at[slot]).wait()

    for b in range(ahead):
        fetch(b, b)
    krow[...] = rope(kv_ref[:, :dim].astype(F32), cos_ref[...], sin_ref[...]).astype(BF16).astype(F32)
    vrow[...] = kv_ref[:, dim:].astype(F32)
    for d in range(n_dev):
        for h in range(per):
            x = rope(q_ref[d, :, h * dim : (h + 1) * dim], cos_ref[...], sin_ref[...])
            qrot[:, d * per + h, :] = x

    def patch(buf, slot, row, p):
        base = pl.multiple_of((p // 16) * 16, 16)
        old = buf[slot, pl.ds(base, 16), :].astype(F32)
        hit = lax.broadcasted_iota(jnp.int32, old.shape, 0) == p - base
        buf[slot, pl.ds(base, 16), :] = jnp.where(hit, row, old).astype(BF16)

    @pl.loop(0, n_seq // 2)
    def _(i):
        work = []
        for j in range(2):
            b = 2 * i + j
            slot = lax.rem(b, nb)
            nxt = b + ahead
            nslot = lax.rem(nxt, nb)

            @pl.when(jnp.logical_and(nxt < n_seq, nxt >= nb))
            def _():
                wait_out(nxt - nb, nslot)

            @pl.when(nxt < n_seq)
            def _():
                fetch(nxt, nslot)

            work.append((b, slot))
        for b, slot in work:
            p = pos_ref[b]
            pltpu.make_async_copy(kc_ref.at[b], kbuf.at[slot], ki.at[slot]).wait()
            patch(kbuf, slot, krow[pl.ds(b, 1), :], p)
            pltpu.make_async_copy(vc_ref.at[b], vbuf.at[slot], vi.at[slot]).wait()
            patch(vbuf, slot, vrow[pl.ds(b, 1), :], p)
        for b, slot in work:
            p = pos_ref[b]
            q = qrot[b].astype(BF16)
            s = lax.dot_general(q, kbuf[slot], (((1,), (1,)), ((), ())), preferred_element_type=F32)
            s = s * (dim ** -0.5)
            ok = lax.broadcasted_iota(jnp.int32, (n_head, length), 1) <= p
            s = jnp.where(ok, s, -jnp.inf)
            e = jnp.exp(s - jnp.max(s, axis=1, keepdims=True))
            prob = (e / jnp.sum(e, axis=1, keepdims=True)).astype(BF16)
            o = jnp.dot(prob, vbuf[slot], preferred_element_type=F32)
            for h in range(n_head):
                orow[h // per, pl.ds(b, 1), (h % per) * dim : (h % per + 1) * dim] = o[h : h + 1]
        for b, slot in work:
            pltpu.make_async_copy(kbuf.at[slot], ko_ref.at[b], ks.at[slot]).start()
            pltpu.make_async_copy(vbuf.at[slot], vo_ref.at[b], vs.at[slot]).start()

    o_ref[...] = orow[...].astype(BF16)
    for b in range(n_seq - nb, n_seq):
        wait_out(b, b % nb)


def attention(q, kv_new, cos, sin, k_cache, v_cache, positions, nb=8, ahead=4):
    n_seq, length, dim = k_cache.shape
    n_head = q.shape[0] * q.shape[2] // dim
    vm = pl.BlockSpec(memory_space=pltpu.VMEM)
    hbm = pl.BlockSpec(memory_space=pltpu.HBM)
    return pl.pallas_call(
        functools.partial(attn_kernel, nb, ahead),
        out_shape=[
            jax.ShapeDtypeStruct(q.shape, BF16),
            jax.ShapeDtypeStruct(k_cache.shape, BF16),
            jax.ShapeDtypeStruct(v_cache.shape, BF16),
        ],
        in_specs=[pl.BlockSpec(memory_space=pltpu.SMEM), vm, vm, vm, vm, hbm, hbm],
        out_specs=[vm, hbm, hbm],
        scratch_shapes=[
            pltpu.VMEM((nb, length, dim), BF16),
            pltpu.VMEM((nb, length, dim), BF16),
            pltpu.VMEM((n_seq, dim), F32),
            pltpu.VMEM((n_seq, dim), F32),
            pltpu.VMEM((n_seq, n_head, dim), F32),
            pltpu.VMEM(q.shape, F32),
            pltpu.SemaphoreType.DMA((nb,)),
            pltpu.SemaphoreType.DMA((nb,)),
            pltpu.SemaphoreType.DMA((nb,)),
            pltpu.SemaphoreType.DMA((nb,)),
        ],
        compiler_params=pltpu.CompilerParams(vmem_limit_bytes=40 * 2**20),
        cost_estimate=pl.CostEstimate(
            flops=4 * 10**10, bytes_accessed=8 * n_seq * length * dim, transcendentals=n_seq * n_head * length
        ),
        name="attention",
    )(positions, q, kv_new, cos, sin, k_cache, v_cache)


def tail_kernel(n_gu, cuts, n_w, *refs):
    keeps, recvs = refs[:n_gu], refs[n_gu : 2 * n_gu]
    (o_ref, wd_hbm, wo_hbm, out_ref, wd, aown, aoth, give, hold, got1, pass_, got2,
     wsem, as_, ar, s1, r1, s2, r2, os_, or_) = refs[2 * n_gu :]
    ix, iy = lax.axis_index("tpx"), lax.axis_index("tpy")
    half = aown.shape[0]
    ny, n_seq = o_ref.shape[0], o_ref.shape[1]
    starts, at = [], 0
    for ref in keeps:
        starts.append((at, ref.shape[2]))
        at += ref.shape[2]
    width = out_ref.shape[1]
    kact, ko = wd_hbm.shape[0], wo_hbm.shape[0]
    partner = iy + 1 - 2 * lax.rem(iy, 2)
    cross = lax.rem(iy + 2, 4)
    core, chip = lax.rem(iy, 2), iy // 2
    peer_x = {"tpx": 1 - ix, "tpy": iy}
    peer_core = {"tpx": ix, "tpy": partner}
    peer_chip = {"tpx": ix, "tpy": cross}

    barrier = pltpu.get_barrier_semaphore()
    others = [(dx, dy) for dx in (1, 0) for dy in range(ny) if dx or dy]

    def shifted(dx, dy):
        return {"tpx": lax.rem(ix + dx, 2), "tpy": lax.rem(iy + dy, ny)}

    for dx, dy in others:
        pl.semaphore_signal(barrier, inc=1, device_id=shifted(dx, dy), device_id_type=MESH)
    step = kact // n_w
    w_loads = []
    for j in range(n_w + 1):
        if j < n_w:
            src, dst = wd_hbm.at[pl.ds(j * step, step)], wd.at[pl.ds(j * step, step)]
        else:
            src, dst = wo_hbm, wd.at[pl.ds(kact, ko)]
        c = pltpu.make_async_copy(src, dst, wsem.at[j])
        c.start()
        w_loads.append(c)

    pl.semaphore_wait(barrier, len(others))

    o_rows = pl.ds(pl.multiple_of(iy * n_seq, n_seq), n_seq)
    o_cols = pl.ds(kact, ko)
    o_copies = []
    for k, (dx, dy) in enumerate(others):
        c = pltpu.make_async_remote_copy(
            src_ref=o_ref.at[lax.rem(iy + dy, ny)],
            dst_ref=(aoth if dx else aown).at[o_rows, o_cols],
            send_sem=os_.at[k],
            recv_sem=or_.at[k],
            device_id=shifted(dx, dy),
            device_id_type=MESH,
        )
        c.start()
        o_copies.append(c)
    aown[o_rows, kact:] = o_ref[iy]

    sends = []
    for r, (r0, rn) in enumerate(cuts):
        rows = pl.ds(r0, rn)
        for g in range(n_gu):
            part = pl.ds(*starts[g])
            gate = (keeps[g][0, rows, :] + recvs[g][0, rows, :]).astype(BF16).astype(F32)
            up = (keeps[g][1, rows, :] + recvs[g][1, rows, :]).astype(BF16).astype(F32)
            aown[rows, part] = (jax.nn.silu(gate) * up).astype(BF16)
        c = pltpu.make_async_remote_copy(
            src_ref=aown.at[rows, pl.ds(0, kact)],
            dst_ref=aoth.at[rows, pl.ds(0, kact)],
            send_sem=as_.at[r],
            recv_sem=ar.at[r],
            device_id=peer_x,
            device_id_type=MESH,
        )
        c.start()
        sends.append(c)
    for c in w_loads:
        c.wait()
    for c in o_copies:
        c.wait_recv()

    blocks = [(half, half)] + [(r0, rn) for r0, rn in cuts]

    def product(lhs, x, c):
        col = pl.ds(pl.multiple_of((x * 2 + c) * width, width), width)
        return jnp.dot(lhs, wd[:, col], preferred_element_type=F32)

    stage1, stage2 = [], []

    def give_block(k, rows, lhs, x):
        give[x, rows, :] = product(lhs, x, 1 - core)
        c = pltpu.make_async_remote_copy(
            src_ref=give.at[x, rows],
            dst_ref=got1.at[x, rows],
            send_sem=s1.at[k, len(stage1[k])],
            recv_sem=r1.at[k, len(stage1[k])],
            device_id=peer_core,
            device_id_type=MESH,
        )
        c.start()
        stage1[k].append(c)

    def reduce_block(k):
        r0, rn = blocks[k]
        rows = pl.ds(r0, rn)
        stage1[k][0].wait_recv()
        pass_[rows, :] = hold[0, rows, :] + got1[1 - chip, rows, :]
        c = pltpu.make_async_remote_copy(
            src_ref=pass_.at[rows],
            dst_ref=got2.at[rows],
            send_sem=s2.at[k],
            recv_sem=r2.at[k],
            device_id=peer_chip,
            device_id_type=MESH,
        )
        c.start()
        stage2.append(c)

    def run_block(k, last):
        r0, rn = blocks[k]
        rows = pl.ds(r0, rn)
        stage1.append([])
        if k == 0:
            lhs = aown[...]
        else:
            sends[k - 1].wait_recv()
            lhs = aoth[rows, :]
        give_block(k, rows, lhs, 1 - chip)
        hold[0, rows, :] = product(lhs, 1 - chip, core)
        if k:
            reduce_block(k - 1)
        give_block(k, rows, lhs, chip)
        if last:
            reduce_block(k)
        hold[1, rows, :] = product(lhs, chip, core)

    def finish_block(k):
        r0, rn = blocks[k]
        rows = pl.ds(r0, rn)
        stage1[k][1].wait_recv()
        partial = hold[1, rows, :] + got1[chip, rows, :]
        stage2[k].wait_recv()
        base = ix * half if k == 0 else (1 - ix) * half + r0
        out_ref[pl.ds(pl.multiple_of(base, 16), rn), :] = partial + got2[rows, :]

    n_blk = len(blocks)
    for k in range(n_blk):
        run_block(k, k == n_blk - 1)
    for k in range(n_blk):
        finish_block(k)
    for c in sends + [c for g in stage1 for c in g] + stage2 + o_copies:
        c.wait_send()


def tail(keeps, recvs, o, rows, width, w_down, w_o):
    n_gu = len(keeps)
    half = keeps[0].shape[1]
    n = w_down.shape[1]
    kdim = w_down.shape[0] + w_o.shape[0]
    cuts = [(0, 64), (64, 32), (96, 16), (112, 16)]
    n_w, n_cut, n_blk = 8, len(cuts), len(cuts) + 1
    vm = pl.BlockSpec(memory_space=pltpu.VMEM)
    hbm = pl.BlockSpec(memory_space=pltpu.HBM)
    dma = pltpu.SemaphoreType.DMA
    return pl.pallas_call(
        functools.partial(tail_kernel, n_gu, cuts, n_w),
        out_shape=jax.ShapeDtypeStruct((rows, width), F32),
        in_specs=[vm] * (2 * n_gu) + [vm] + [hbm] * 2,
        out_specs=vm,
        scratch_shapes=[
            pltpu.VMEM((kdim, n), BF16),
            pltpu.VMEM((half, kdim), BF16),
            pltpu.VMEM((half, kdim), BF16),
            pltpu.VMEM((2, rows, width), F32),
            pltpu.VMEM((2, rows, width), F32),
            pltpu.VMEM((2, rows, width), F32),
            pltpu.VMEM((rows, width), F32),
            pltpu.VMEM((rows, width), F32),
            dma((n_w + 1,)),
            dma((n_cut,)),
            dma((n_cut,)),
            dma((n_blk, 2)),
            dma((n_blk, 2)),
            dma((n_blk,)),
            dma((n_blk,)),
            dma((7,)),
            dma((7,)),
        ],
        compiler_params=pltpu.CompilerParams(collective_id=1, has_side_effects=True, vmem_limit_bytes=40 * 2**20),
        cost_estimate=pl.CostEstimate(flops=2 * rows * kdim * n, bytes_accessed=2 * kdim * n, transcendentals=0),
        name="tail",
    )(*keeps, *recvs, o, w_down, w_o)


def solution(mesh):
    x_size = mesh.shape["tpx"]
    y_size = mesh.shape["tpy"]
    hidden_spec = P("dp", ("tpx", "tpy"))
    cache_spec = P(("dp", "tpx", "tpy"), None, None)
    in_specs = (hidden_spec, P(("tpx", "tpy")), P("tpx", "tpy"), P("tpx", None), P("tpx", None), P("tpx", "tpy"), P("tpx", "tpy"), P("tpy", "tpx"), P("tpy", "tpx"), cache_spec, cache_spec, P(("dp", "tpx", "tpy")))
    out_specs = (hidden_spec, cache_spec, cache_spec)
    swap_x = [(0, 1), (1, 0)]
    ge, sizes = 512, (768, 1024, 1024, 768)

    def device_step(hidden, ln_scale, w_q, w_k, w_v, w_gate, w_up, w_o, w_down, k_cache, v_cache, positions):
        q, kv_new, keep_e, recv_e, u, send, keep_0 = front(
            x_size, y_size, ge, sizes[0], hidden, ln_scale, w_q, w_k, w_v, w_gate, w_up
        )
        keep, recv = [keep_e, keep_0], [recv_e]
        at = ge + sizes[0]
        for c, n in enumerate(sizes):
            if c:
                send, k = gate_up(u, w_gate, w_up, at, n, 256)
                keep.append(k)
                at += n
            recv.append(lax.ppermute(send, "tpx", swap_x))

        cos_tab, sin_tab = rope_tables(positions, k_cache.shape[2])
        o, k_all, v_all = attention(q, kv_new, cos_tab, sin_tab, k_cache, v_cache, positions)
        total = tail(keep, recv, o, *hidden.shape, w_down, w_o)
        hidden_out = (hidden.astype(F32) + total).astype(BF16)
        return hidden_out, k_all, v_all

    return jax.shard_map(device_step, mesh=mesh, in_specs=in_specs, out_specs=out_specs, check_vma=False)
```

```python
import functools

import jax
import jax.numpy as jnp
from jax import lax
from jax.experimental import pallas as pl
from jax.experimental.pallas import tpu as pltpu
from jax.sharding import PartitionSpec as P


LN_EPS = 1e-6
ROPE_BASE = 10000.0
MESH = pl.DeviceIdType.MESH
F32 = jnp.float32
BF16 = jnp.bfloat16


def rope_tables(positions, head_dim):
    half_dim = head_dim // 2
    inv_freq = ROPE_BASE ** (-(jnp.arange(half_dim, dtype=F32) * 2.0 / head_dim))
    angles = positions.astype(F32)[:, None] * inv_freq[None, :]
    return jnp.cos(angles), jnp.sin(angles)


def rope(x, cos, sin):
    half = x.shape[-1] // 2
    lead, tail = x[:, :half], x[:, half:]
    return jnp.concatenate([lead * cos - tail * sin, lead * sin + tail * cos], axis=-1)


def front_kernel(nx, ny, ge, gc, h_ref, sc_ref, wq_hbm, wk_hbm, wv_hbm, wg_hbm, wu_hbm,
                 q_hbm, kv_hbm, ke_hbm, re_hbm, u_hbm, gs_hbm, gk_hbm,
                 hbuf, scbuf, stat, cols, u_ref, wq, wkv, wgu, qs, qr, qo, kvs, kvr, es, ke, gs, gk, qn, qall, qf, kvn,
                 wsem, hs, hr, ss, sr, ts, tr, qss, qrs, ls, as_, ar, outs):
    ix, iy = lax.axis_index("tpx"), lax.axis_index("tpy")
    rows, width = h_ref.shape
    n_dev = nx * ny
    half = rows // 2
    n_seq = half // ny
    dim = wk_hbm.shape[1]
    gw = ge + gc
    partner = iy + 1 - 2 * lax.rem(iy, 2)
    cross = lax.rem(iy + 2, ny)
    diag = lax.rem(partner + 2, ny)
    me = ix * ny + iy
    peer_x = {"tpx": 1 - ix, "tpy": iy}

    def remote(src, dst, send, recv, dev):
        return pltpu.make_async_remote_copy(
            src_ref=src, dst_ref=dst, send_sem=send, recv_sem=recv, device_id=dev, device_id_type=MESH
        )

    loads = [
        pltpu.make_async_copy(wq_hbm, wq, wsem.at[0]),
        pltpu.make_async_copy(wk_hbm, wkv.at[0], wsem.at[1]),
        pltpu.make_async_copy(wv_hbm, wkv.at[1], wsem.at[2]),
        pltpu.make_async_copy(wg_hbm.at[:, 0:gw], wgu.at[0], wsem.at[3]),
        pltpu.make_async_copy(wu_hbm.at[:, 0:gw], wgu.at[1], wsem.at[4]),
    ]
    for c in loads:
        c.start()

    others = [(dx, dy) for dx in range(nx) for dy in range(ny) if dx or dy]
    barrier = pltpu.get_barrier_semaphore()
    for dx, dy in others:
        pl.semaphore_signal(
            barrier,
            inc=1,
            device_id={"tpx": lax.rem(ix + dx, nx), "tpy": lax.rem(iy + dy, ny)},
            device_id_type=MESH,
        )
    hf = h_ref[...].astype(F32)
    total = jnp.sum(hf, axis=1, keepdims=True)
    dev = hf - total / width
    spread = jnp.sum(dev * dev, axis=1, keepdims=True)
    lane = lax.broadcasted_iota(jnp.int32, (rows, 128), 1)
    packed = jnp.where(lane == 0, total, jnp.where(lane == 1, spread, 0.0))
    stat[me] = jnp.transpose(packed)[:2]
    pl.semaphore_wait(barrier, n_dev - 1)

    chunks = [(0, 32), (32, half - 32), (half, half // 2), (half + half // 2, half // 2)]
    n_ch = len(chunks)

    def nat(j):
        r0, rn = chunks[j]
        base = (1 - ix) * half + r0 if r0 < half else ix * half + r0 - half
        return pl.ds(pl.multiple_of(base, 32), rn)

    def perm(j):
        return pl.ds(*chunks[j])

    def h_copy(j, dst_y, k):
        return remote(h_ref.at[nat(j)], hbuf.at[iy, perm(j)], hs.at[k, j], hr.at[k, j], {"tpx": ix, "tpy": dst_y})

    to_cross = [h_copy(j, cross, 0) for j in range(n_ch)]
    to_partner = [h_copy(j, partner, 1) for j in range(n_ch)]
    stat_copies = []
    for k, (dx, dy) in enumerate(others):
        c = remote(
            stat.at[me], stat.at[me], ts.at[k], tr.at[k],
            {"tpx": lax.rem(ix + dx, nx), "tpy": lax.rem(iy + dy, ny)},
        )
        c.start()
        stat_copies.append(c)
    to_cross[0].start()
    to_diag = h_copy(0, diag, 2)
    to_diag.start()
    for c in to_partner:
        c.start()

    sc_copies = []
    for k, dst in enumerate((cross, partner, diag)):
        c = remote(sc_ref, scbuf.at[iy], ss.at[k], sr.at[k], {"tpx": ix, "tpy": dst})
        c.start()
        sc_copies.append(c)
    for c in to_cross[1:]:
        c.start()

    forward = [to_diag]

    def relay(j):
        to_cross[j].wait_recv()
        part = hbuf.at[cross, perm(j)]
        c = remote(part, part, hs.at[2, j], hr.at[2, j], {"tpx": ix, "tpy": partner})
        c.start()
        forward.append(c)

    to_cross[0].wait_recv()
    for c in stat_copies:
        c.wait_recv()
    sums = [stat[d, 0:1, :] for d in range(n_dev)]
    sprd = [stat[d, 1:2, :] for d in range(n_dev)]
    mean = functools.reduce(jnp.add, sums) / (width * n_dev)
    m2 = functools.reduce(jnp.add, sprd)
    for d in range(n_dev):
        gap = sums[d] / width - mean
        m2 = m2 + width * gap * gap
    rs = lax.rsqrt(m2 / (width * n_dev) + LN_EPS)
    sub = lax.broadcasted_iota(jnp.int32, (128, rows), 0)
    cols[...] = jnp.transpose(jnp.where(sub == 0, mean, jnp.where(sub == 1, rs, 0.0)))
    for c in sc_copies:
        c.wait_recv()

    def emit(block, scale, owner, j):
        stats = cols[nat(j), :]
        u = ((block.astype(F32) - stats[:, 0:1]) * stats[:, 1:2] * scale).astype(BF16)
        u_ref[perm(j), pl.ds(pl.multiple_of(owner * width, width), width)] = u

    def normalise(j):
        emit(h_ref[nat(j), :], sc_ref[...], iy, j)
        to_partner[j].wait_recv()
        emit(hbuf[partner, perm(j), :], scbuf[partner], partner, j)
        emit(hbuf[cross, perm(j), :], scbuf[cross], cross, j)
        forward[j].wait_recv()
        emit(hbuf[diag, perm(j), :], scbuf[diag], diag, j)

    def dot(a, b):
        return jnp.dot(a, b, preferred_element_type=F32)

    q_copies = []
    for j in range(n_ch):
        if 0 < j < n_ch - 1:
            relay(j + 1)
        normalise(j)
        if j < n_ch // 2:
            if j == 0:
                loads[0].wait()
            qs[perm(j), :] = dot(u_ref[perm(j), :], wq[...])
            c = remote(qs.at[perm(j)], qr.at[perm(j)], qss.at[j], qrs.at[j], peer_x)
            c.start()
            q_copies.append(c)
        if j == 0:
            relay(1)
    loads[1].wait()
    loads[2].wait()
    oth_rows = u_ref[pl.ds(pl.multiple_of(iy * n_seq, n_seq), n_seq), :]
    own_rows = u_ref[pl.ds(pl.multiple_of(half + iy * n_seq, n_seq), n_seq), :]
    for k in range(2):
        kvs[:, k * dim : (k + 1) * dim] = dot(oth_rows, wkv[k])
    kv_copy = remote(kvs, kvr, ls.at[0], ls.at[1], peer_x)
    kv_copy.start()
    u_out = pltpu.make_async_copy(u_ref, u_hbm, outs.at[0])
    u_out.start()
    loads[3].wait()
    loads[4].wait()
    for k in range(2):
        y = dot(u_ref[...], wgu[k, :, 0:ge])
        es[k] = y[:half]
        ke[k] = y[half:]
    e_copy = remote(es, re_hbm, ls.at[2], ls.at[3], peer_x)
    e_copy.start()
    ke_out = pltpu.make_async_copy(ke, ke_hbm, outs.at[3])
    ke_out.start()
    qo[...] = dot(u_ref[pl.ds(half, half), :], wq[...])
    own_kv = [dot(own_rows, wkv[k]) for k in range(2)]

    def gate_up_part(lo, hi):
        for k in range(2):
            y = dot(u_ref[...], wgu[k, :, ge + lo : ge + hi])
            gs[k, :, lo:hi] = y[:half]
            gk[k, :, lo:hi] = y[half:]

    gate_up_part(0, gc // 2)
    for j in range(n_ch // 2):
        q_copies[j].wait_recv()
        qn[perm(j), :] = (qo[perm(j), :] + qr[perm(j), :]).astype(BF16)
    q_sends = []
    for k in range(1, ny):
        d = lax.rem(iy + k, ny)
        c = remote(
            qn.at[pl.ds(pl.multiple_of(d * n_seq, n_seq), n_seq)], qall.at[iy],
            as_.at[k - 1], ar.at[k - 1], {"tpx": ix, "tpy": d},
        )
        c.start()
        q_sends.append(c)
    gate_up_part(gc // 2, gc)
    g_out = [pltpu.make_async_copy(gs, gs_hbm, outs.at[1]), pltpu.make_async_copy(gk, gk_hbm, outs.at[2])]
    for c in g_out:
        c.start()
    kv_copy.wait_recv()
    for k in range(2):
        sl = slice(k * dim, (k + 1) * dim)
        kvn[:, sl] = (own_kv[k] + kvr[:, sl]).astype(BF16)
    kv_out = pltpu.make_async_copy(kvn, kv_hbm, outs.at[4])
    kv_out.start()
    qf[iy] = qn[pl.ds(pl.multiple_of(iy * n_seq, n_seq), n_seq), :].astype(F32)
    for k in range(1, ny):
        q_sends[k - 1].wait_recv()
        src = lax.rem(iy + ny - k, ny)
        qf[src] = qall[src].astype(F32)
    q_out = pltpu.make_async_copy(qf, q_hbm, outs.at[5])
    q_out.start()
    e_copy.wait_recv()
    for c in to_cross + to_partner + forward + sc_copies + stat_copies + q_copies + q_sends + [kv_copy, e_copy]:
        c.wait_send()
    for c in [u_out, ke_out, kv_out, q_out] + g_out:
        c.wait()


def front(nx, ny, ge, gc, hidden, ln_scale, w_q, w_k, w_v, w_gate, w_up):
    rows, width = hidden.shape
    half = rows // 2
    n_dev, n_seq = nx * ny, rows // (nx * ny)
    kdim, nq = w_q.shape
    dim = w_k.shape[1]
    vm = pl.BlockSpec(memory_space=pltpu.VMEM)
    hbm = pl.BlockSpec(memory_space=pltpu.HBM)
    dma = pltpu.SemaphoreType.DMA
    sds = jax.ShapeDtypeStruct
    return pl.pallas_call(
        functools.partial(front_kernel, nx, ny, ge, gc),
        out_shape=[
            sds((ny, n_seq, nq), F32),
            sds((n_seq, 2 * dim), BF16),
            sds((2, half, ge), F32),
            sds((2, half, ge), F32),
            sds((rows, kdim), BF16),
            sds((2, half, gc), F32),
            sds((2, half, gc), F32),
        ],
        in_specs=[vm, vm] + [hbm] * 5,
        out_specs=[hbm] * 7,
        scratch_shapes=[
            pltpu.VMEM((ny, rows, width), BF16),
            pltpu.VMEM((ny, 1, width), F32),
            pltpu.VMEM((n_dev, 2, rows), F32),
            pltpu.VMEM((rows, 128), F32),
            pltpu.VMEM((rows, kdim), BF16),
            pltpu.VMEM((kdim, nq), BF16),
            pltpu.VMEM((2, kdim, dim), BF16),
            pltpu.VMEM((2, kdim, ge + gc), BF16),
            pltpu.VMEM((half, nq), F32),
            pltpu.VMEM((half, nq), F32),
            pltpu.VMEM((half, nq), F32),
            pltpu.VMEM((n_seq, 2 * dim), F32),
            pltpu.VMEM((n_seq, 2 * dim), F32),
            pltpu.VMEM((2, half, ge), F32),
            pltpu.VMEM((2, half, ge), F32),
            pltpu.VMEM((2, half, gc), F32),
            pltpu.VMEM((2, half, gc), F32),
            pltpu.VMEM((half, nq), BF16),
            pltpu.VMEM((ny, n_seq, nq), BF16),
            pltpu.VMEM((ny, n_seq, nq), F32),
            pltpu.VMEM((n_seq, 2 * dim), BF16),
            dma((5,)),
            dma((3, 4)),
            dma((3, 4)),
            dma((3,)),
            dma((3,)),
            dma((n_dev - 1,)),
            dma((n_dev - 1,)),
            dma((2,)),
            dma((2,)),
            dma((4,)),
            dma((ny - 1,)),
            dma((ny - 1,)),
            dma((6,)),
        ],
        compiler_params=pltpu.CompilerParams(collective_id=0, has_side_effects=True, vmem_limit_bytes=56 * 2**20),
        cost_estimate=pl.CostEstimate(flops=2 * rows * kdim * nq, bytes_accessed=2 * kdim * nq, transcendentals=0),
        name="front",
    )(hidden, ln_scale.reshape(1, width), w_q, w_k, w_v, w_gate, w_up)


def gu_kernel(u_ref, wg_ref, wu_ref, send, keep):
    half = u_ref.shape[0] // 2
    for k, w_ref in enumerate((wg_ref, wu_ref)):
        y = jnp.dot(u_ref[...], w_ref[...], preferred_element_type=F32)
        send[k] = y[:half]
        keep[k] = y[half:]


def gate_up(u, w_gate, w_up, start, cols, blk):
    rows, kdim = u.shape
    half = rows // 2
    first = start // blk
    shape = jax.ShapeDtypeStruct((2, half, cols), F32)
    wspec = pl.BlockSpec((kdim, blk), lambda i: (0, i + first))
    ospec = pl.BlockSpec((2, half, blk), lambda i: (0, 0, i))
    return pl.pallas_call(
        gu_kernel,
        grid=(cols // blk,),
        out_shape=[shape, shape],
        in_specs=[pl.BlockSpec((rows, kdim), lambda i: (0, 0)), wspec, wspec],
        out_specs=[ospec, ospec],
        compiler_params=pltpu.CompilerParams(vmem_limit_bytes=56 * 2**20),
        cost_estimate=pl.CostEstimate(
            flops=4 * rows * kdim * cols, bytes_accessed=4 * kdim * cols, transcendentals=0
        ),
        name="gate_up",
    )(u, w_gate, w_up)


def attn_kernel(nb, ahead, pos_ref, q_ref, kv_ref, cos_ref, sin_ref, kc_ref, vc_ref,
                o_ref, ko_ref, vo_ref, kbuf, vbuf, krow, vrow, qrot, orow, ki, vi, ks, vs):
    n_seq, n_head, dim = qrot.shape
    n_dev = q_ref.shape[0]
    per = n_head // n_dev
    length = kbuf.shape[1]

    def fetch(b, slot):
        pltpu.make_async_copy(kc_ref.at[b], kbuf.at[slot], ki.at[slot]).start()
        pltpu.make_async_copy(vc_ref.at[b], vbuf.at[slot], vi.at[slot]).start()

    def wait_out(b, slot):
        pltpu.make_async_copy(kbuf.at[slot], ko_ref.at[b], ks.at[slot]).wait()
        pltpu.make_async_copy(vbuf.at[slot], vo_ref.at[b], vs.at[slot]).wait()

    for b in range(ahead):
        fetch(b, b)
    krow[...] = rope(kv_ref[:, :dim].astype(F32), cos_ref[...], sin_ref[...]).astype(BF16).astype(F32)
    vrow[...] = kv_ref[:, dim:].astype(F32)
    for d in range(n_dev):
        for h in range(per):
            x = rope(q_ref[d, :, h * dim : (h + 1) * dim], cos_ref[...], sin_ref[...])
            qrot[:, d * per + h, :] = x

    def patch(buf, slot, row, p):
        base = pl.multiple_of((p // 16) * 16, 16)
        old = buf[slot, pl.ds(base, 16), :].astype(F32)
        hit = lax.broadcasted_iota(jnp.int32, old.shape, 0) == p - base
        buf[slot, pl.ds(base, 16), :] = jnp.where(hit, row, old).astype(BF16)

    @pl.loop(0, n_seq // 2)
    def _(i):
        work = []
        for j in range(2):
            b = 2 * i + j
            slot = lax.rem(b, nb)
            nxt = b + ahead
            nslot = lax.rem(nxt, nb)

            @pl.when(jnp.logical_and(nxt < n_seq, nxt >= nb))
            def _():
                wait_out(nxt - nb, nslot)

            @pl.when(nxt < n_seq)
            def _():
                fetch(nxt, nslot)

            work.append((b, slot))
        for b, slot in work:
            p = pos_ref[b]
            pltpu.make_async_copy(kc_ref.at[b], kbuf.at[slot], ki.at[slot]).wait()
            patch(kbuf, slot, krow[pl.ds(b, 1), :], p)
            pltpu.make_async_copy(vc_ref.at[b], vbuf.at[slot], vi.at[slot]).wait()
            patch(vbuf, slot, vrow[pl.ds(b, 1), :], p)
        for b, slot in work:
            p = pos_ref[b]
            q = qrot[b].astype(BF16)
            s = lax.dot_general(q, kbuf[slot], (((1,), (1,)), ((), ())), preferred_element_type=F32)
            s = s * (dim ** -0.5)
            ok = lax.broadcasted_iota(jnp.int32, (n_head, length), 1) <= p
            s = jnp.where(ok, s, -jnp.inf)
            e = jnp.exp(s - jnp.max(s, axis=1, keepdims=True))
            prob = (e / jnp.sum(e, axis=1, keepdims=True)).astype(BF16)
            o = jnp.dot(prob, vbuf[slot], preferred_element_type=F32)
            for h in range(n_head):
                orow[h // per, pl.ds(b, 1), (h % per) * dim : (h % per + 1) * dim] = o[h : h + 1]
        for b, slot in work:
            pltpu.make_async_copy(kbuf.at[slot], ko_ref.at[b], ks.at[slot]).start()
            pltpu.make_async_copy(vbuf.at[slot], vo_ref.at[b], vs.at[slot]).start()

    o_ref[...] = orow[...].astype(BF16)
    for b in range(n_seq - nb, n_seq):
        wait_out(b, b % nb)


def attention(q, kv_new, cos, sin, k_cache, v_cache, positions, nb=8, ahead=4):
    n_seq, length, dim = k_cache.shape
    n_head = q.shape[0] * q.shape[2] // dim
    vm = pl.BlockSpec(memory_space=pltpu.VMEM)
    hbm = pl.BlockSpec(memory_space=pltpu.HBM)
    return pl.pallas_call(
        functools.partial(attn_kernel, nb, ahead),
        out_shape=[
            jax.ShapeDtypeStruct(q.shape, BF16),
            jax.ShapeDtypeStruct(k_cache.shape, BF16),
            jax.ShapeDtypeStruct(v_cache.shape, BF16),
        ],
        in_specs=[pl.BlockSpec(memory_space=pltpu.SMEM), vm, vm, vm, vm, hbm, hbm],
        out_specs=[vm, hbm, hbm],
        scratch_shapes=[
            pltpu.VMEM((nb, length, dim), BF16),
            pltpu.VMEM((nb, length, dim), BF16),
            pltpu.VMEM((n_seq, dim), F32),
            pltpu.VMEM((n_seq, dim), F32),
            pltpu.VMEM((n_seq, n_head, dim), F32),
            pltpu.VMEM(q.shape, F32),
            pltpu.SemaphoreType.DMA((nb,)),
            pltpu.SemaphoreType.DMA((nb,)),
            pltpu.SemaphoreType.DMA((nb,)),
            pltpu.SemaphoreType.DMA((nb,)),
        ],
        compiler_params=pltpu.CompilerParams(vmem_limit_bytes=40 * 2**20),
        cost_estimate=pl.CostEstimate(
            flops=4 * 10**10, bytes_accessed=8 * n_seq * length * dim, transcendentals=n_seq * n_head * length
        ),
        name="attention",
    )(positions, q, kv_new, cos, sin, k_cache, v_cache)


def tail_kernel(n_gu, cuts, n_w, *refs):
    keeps, recvs = refs[:n_gu], refs[n_gu : 2 * n_gu]
    (o_ref, wd_hbm, wo_hbm, out_ref, wd, aown, aoth, give, hold, got1, pass_, got2,
     wsem, as_, ar, s1, r1, s2, r2, os_, or_, ready) = refs[2 * n_gu :]
    ix, iy = lax.axis_index("tpx"), lax.axis_index("tpy")
    half = aown.shape[0]
    ny, n_seq = o_ref.shape[0], o_ref.shape[1]
    starts, at = [], 0
    for ref in keeps:
        starts.append((at, ref.shape[2]))
        at += ref.shape[2]
    width = out_ref.shape[1]
    kact, ko = wd_hbm.shape[0], wo_hbm.shape[0]
    partner = iy + 1 - 2 * lax.rem(iy, 2)
    cross = lax.rem(iy + 2, 4)
    core, chip = lax.rem(iy, 2), iy // 2
    peer_x = {"tpx": 1 - ix, "tpy": iy}
    peer_core = {"tpx": ix, "tpy": partner}
    peer_chip = {"tpx": ix, "tpy": cross}

    barrier = pltpu.get_barrier_semaphore()
    neighbours = (peer_x, peer_core, peer_chip)
    for d in neighbours:
        pl.semaphore_signal(barrier, inc=1, device_id=d, device_id_type=MESH)
    step = kact // n_w
    w_loads = []
    for j in range(n_w + 1):
        if j < n_w:
            src, dst = wd_hbm.at[pl.ds(j * step, step)], wd.at[pl.ds(j * step, step)]
        else:
            src, dst = wo_hbm, wd.at[pl.ds(kact, ko)]
        c = pltpu.make_async_copy(src, dst, wsem.at[j])
        c.start()
        w_loads.append(c)

    sends = []

    def make_act(r):
        rows = pl.ds(*cuts[r])
        for g in range(n_gu):
            part = pl.ds(*starts[g])
            gate = (keeps[g][0, rows, :] + recvs[g][0, rows, :]).astype(BF16).astype(F32)
            up = (keeps[g][1, rows, :] + recvs[g][1, rows, :]).astype(BF16).astype(F32)
            aown[rows, part] = (jax.nn.silu(gate) * up).astype(BF16)

    def send_act(r):
        rows = pl.ds(*cuts[r])
        c = pltpu.make_async_remote_copy(
            src_ref=aown.at[rows, pl.ds(0, kact)],
            dst_ref=aoth.at[rows, pl.ds(0, kact)],
            send_sem=as_.at[r],
            recv_sem=ar.at[r],
            device_id=peer_x,
            device_id_type=MESH,
        )
        c.start()
        sends.append(c)

    o_rows = pl.ds(pl.multiple_of(iy * n_seq, n_seq), n_seq)
    o_cols = pl.ds(kact, ko)
    diag = lax.rem(partner + 2, ny)
    o_own, o_oth = [], []

    def send_o(dst, cross_x):
        k = len(o_own) + len(o_oth)
        c = pltpu.make_async_remote_copy(
            src_ref=o_ref.at[dst],
            dst_ref=(aoth if cross_x else aown).at[o_rows, o_cols],
            send_sem=os_.at[k],
            recv_sem=or_.at[k],
            device_id={"tpx": 1 - ix if cross_x else ix, "tpy": dst},
            device_id_type=MESH,
        )
        c.start()
        (o_oth if cross_x else o_own).append(c)

    def tell(k):
        for d in neighbours:
            pl.semaphore_signal(ready.at[k], inc=1, device_id=d, device_id_type=MESH)

    make_act(0)
    pl.semaphore_wait(barrier, len(neighbours))
    send_o(iy, True)
    tell(0)
    send_act(0)
    send_o(partner, False)
    send_o(cross, False)
    pl.semaphore_wait(ready.at[0], len(neighbours))
    tell(1)
    send_o(partner, True)
    send_o(cross, True)
    send_o(diag, False)
    pl.semaphore_wait(ready.at[1], len(neighbours))
    send_o(diag, True)
    aown[o_rows, kact:] = o_ref[iy]
    for r in range(1, len(cuts)):
        make_act(r)
        send_act(r)
    for c in w_loads:
        c.wait()
    for c in o_own:
        c.wait_recv()

    blocks = [(half, half)] + [(r0, rn) for r0, rn in cuts]

    def product(lhs, x, c):
        col = pl.ds(pl.multiple_of((x * 2 + c) * width, width), width)
        return jnp.dot(lhs, wd[:, col], preferred_element_type=F32)

    stage1, stage2 = [], []

    def give_block(k, rows, lhs, x):
        give[x, rows, :] = product(lhs, x, 1 - core)
        c = pltpu.make_async_remote_copy(
            src_ref=give.at[x, rows],
            dst_ref=got1.at[x, rows],
            send_sem=s1.at[k, len(stage1[k])],
            recv_sem=r1.at[k, len(stage1[k])],
            device_id=peer_core,
            device_id_type=MESH,
        )
        c.start()
        stage1[k].append(c)

    def reduce_block(k):
        r0, rn = blocks[k]
        rows = pl.ds(r0, rn)
        stage1[k][0].wait_recv()
        pass_[rows, :] = hold[0, rows, :] + got1[1 - chip, rows, :]
        c = pltpu.make_async_remote_copy(
            src_ref=pass_.at[rows],
            dst_ref=got2.at[rows],
            send_sem=s2.at[k],
            recv_sem=r2.at[k],
            device_id=peer_chip,
            device_id_type=MESH,
        )
        c.start()
        stage2.append(c)

    def run_block(k, last):
        r0, rn = blocks[k]
        rows = pl.ds(r0, rn)
        stage1.append([])
        if k == 0:
            lhs = aown[...]
        else:
            if k == 1:
                for c in o_oth:
                    c.wait_recv()
            sends[k - 1].wait_recv()
            lhs = aoth[rows, :]
        give_block(k, rows, lhs, 1 - chip)
        hold[0, rows, :] = product(lhs, 1 - chip, core)
        if k:
            reduce_block(k - 1)
        give_block(k, rows, lhs, chip)
        if last:
            reduce_block(k)
        hold[1, rows, :] = product(lhs, chip, core)

    def finish_block(k):
        r0, rn = blocks[k]
        rows = pl.ds(r0, rn)
        stage1[k][1].wait_recv()
        partial = hold[1, rows, :] + got1[chip, rows, :]
        stage2[k].wait_recv()
        base = ix * half if k == 0 else (1 - ix) * half + r0
        out_ref[pl.ds(pl.multiple_of(base, 16), rn), :] = partial + got2[rows, :]

    n_blk = len(blocks)
    for k in range(n_blk):
        run_block(k, k == n_blk - 1)
    for k in range(n_blk):
        finish_block(k)
    for c in sends + [c for g in stage1 for c in g] + stage2 + o_own + o_oth:
        c.wait_send()


def tail(keeps, recvs, o, rows, width, w_down, w_o):
    n_gu = len(keeps)
    half = keeps[0].shape[1]
    n = w_down.shape[1]
    kdim = w_down.shape[0] + w_o.shape[0]
    cuts = [(0, 64), (64, 32), (96, 16), (112, 16)]
    n_w, n_cut, n_blk = 8, len(cuts), len(cuts) + 1
    vm = pl.BlockSpec(memory_space=pltpu.VMEM)
    hbm = pl.BlockSpec(memory_space=pltpu.HBM)
    dma = pltpu.SemaphoreType.DMA
    return pl.pallas_call(
        functools.partial(tail_kernel, n_gu, cuts, n_w),
        out_shape=jax.ShapeDtypeStruct((rows, width), F32),
        in_specs=[vm] * (2 * n_gu) + [vm] + [hbm] * 2,
        out_specs=vm,
        scratch_shapes=[
            pltpu.VMEM((kdim, n), BF16),
            pltpu.VMEM((half, kdim), BF16),
            pltpu.VMEM((half, kdim), BF16),
            pltpu.VMEM((2, rows, width), F32),
            pltpu.VMEM((2, rows, width), F32),
            pltpu.VMEM((2, rows, width), F32),
            pltpu.VMEM((rows, width), F32),
            pltpu.VMEM((rows, width), F32),
            dma((n_w + 1,)),
            dma((n_cut,)),
            dma((n_cut,)),
            dma((n_blk, 2)),
            dma((n_blk, 2)),
            dma((n_blk,)),
            dma((n_blk,)),
            dma((7,)),
            dma((7,)),
            pltpu.SemaphoreType.REGULAR((2,)),
        ],
        compiler_params=pltpu.CompilerParams(collective_id=1, has_side_effects=True, vmem_limit_bytes=40 * 2**20),
        cost_estimate=pl.CostEstimate(flops=2 * rows * kdim * n, bytes_accessed=2 * kdim * n, transcendentals=0),
        name="tail",
    )(*keeps, *recvs, o, w_down, w_o)


def solution(mesh):
    x_size = mesh.shape["tpx"]
    y_size = mesh.shape["tpy"]
    hidden_spec = P("dp", ("tpx", "tpy"))
    cache_spec = P(("dp", "tpx", "tpy"), None, None)
    in_specs = (hidden_spec, P(("tpx", "tpy")), P("tpx", "tpy"), P("tpx", None), P("tpx", None), P("tpx", "tpy"), P("tpx", "tpy"), P("tpy", "tpx"), P("tpy", "tpx"), cache_spec, cache_spec, P(("dp", "tpx", "tpy")))
    out_specs = (hidden_spec, cache_spec, cache_spec)
    swap_x = [(0, 1), (1, 0)]
    ge, sizes = 512, (768, 1024, 1024, 768)

    def device_step(hidden, ln_scale, w_q, w_k, w_v, w_gate, w_up, w_o, w_down, k_cache, v_cache, positions):
        q, kv_new, keep_e, recv_e, u, send, keep_0 = front(
            x_size, y_size, ge, sizes[0], hidden, ln_scale, w_q, w_k, w_v, w_gate, w_up
        )
        keep, recv = [keep_e, keep_0], [recv_e]
        at = ge + sizes[0]
        for c, n in enumerate(sizes):
            if c:
                send, k = gate_up(u, w_gate, w_up, at, n, 256)
                keep.append(k)
                at += n
            recv.append(lax.ppermute(send, "tpx", swap_x))

        cos_tab, sin_tab = rope_tables(positions, k_cache.shape[2])
        o, k_all, v_all = attention(q, kv_new, cos_tab, sin_tab, k_cache, v_cache, positions)
        total = tail(keep, recv, o, *hidden.shape, w_down, w_o)
        hidden_out = (hidden.astype(F32) + total).astype(BF16)
        return hidden_out, k_all, v_all

    return jax.shard_map(device_step, mesh=mesh, in_specs=in_specs, out_specs=out_specs, check_vma=False)
```
